128 devices in a mesh: left: 16 (over z, x), right: 8 (over y, core).
Axes of the slice: x: 4, y: 4, z: 4, core: 2. Of those that a mesh axis runs over, the one named last changes fastest.
Arguments:
- species: float32 [4, 512, 256, 256], P(None, None, 'left', 'right'), may hold values from -6 to 6
- coupling: float32 [4, 4], replicated, may hold values from -4 to 4
- symbol_x: float32 [512], replicated, may hold values from 0.3 to 3
- symbol_y: float32 [256], replicated, may hold values from 0.3 to 3
- symbol_z: float32 [256], replicated, may hold values from 0.3 to 3
Outputs:
- modes: float32 [4, 512, 256, 256], P(None, 'left', 'right')
The draws below stay inside these ranges and needn't reach their ends.
All inputs are finite; a program needn't handle non-finite values.
Results may differ from the reference program's by a relative error of at most 0.000071.
Values sent between devices are 32-bit elements; how exact they have to be, the bound alone decides.
A program may use at most 128 MiB of HBM per device.

```python
import jax
import jax.numpy as jnp
from jax import lax

GRID_X = 512
GRID_Y = 256
GRID_Z = 256
FIELDS = 4


def block_scale(stream_key, dims, pieces, smallest, top_value):
    def one(position, blocks):
        draws = jax.random.uniform(jax.random.fold_in(jax.random.fold_in(stream_key, 6), position), (blocks,), jnp.float32, smallest / len(pieces), top_value / len(pieces))
        return jnp.repeat(jnp.exp(draws), dims[position] // blocks).reshape((-1,) + (1,) * (len(dims) - position - 1))

    level = one(*pieces[0])
    for cut in pieces[1:]:
        level = level * one(*cut)
    return level


def noise(own_key, dims, deviation, reach, cuts=(), dtype=jnp.bfloat16):
    gain = block_scale(own_key, dims, cuts, -0.22, 0.18) if cuts else 1.0
    array = jax.random.normal(own_key, dims, jnp.float32) * deviation * gain
    return jnp.minimum(jnp.maximum(array, -reach), reach).astype(dtype)


def setup_inputs(seed: int = 0) -> dict:
    streams_of = jax.random.split(jax.random.key(seed), 6)
    species = noise(streams_of[0], (FIELDS, GRID_X, GRID_Y, GRID_Z), 1.0, 6.0, ((2, 16), (3, 8)), jnp.float32)
    coupling = noise(streams_of[1], (FIELDS, FIELDS), 0.7, 4.0, (), jnp.float32)
    symbol_x = jnp.clip(jax.random.uniform(streams_of[2], (GRID_X,), jnp.float32, 0.3, 3.0), 0.3, 3.0)
    symbol_y = jnp.clip(jax.random.uniform(streams_of[3], (GRID_Y,), jnp.float32, 0.3, 3.0), 0.3, 3.0)
    symbol_z = jnp.clip(jax.random.uniform(streams_of[4], (GRID_Z,), jnp.float32, 0.3, 3.0), 0.3, 3.0)
    return {"species": species, "coupling": coupling, "symbol_x": symbol_x, "symbol_y": symbol_y, "symbol_z": symbol_z}


def basis_table(count):
    rank = jnp.arange(count)
    angle = (2.0 * jnp.pi / count) * ((rank[:, None] * rank[None, :]) % count).astype(jnp.float32)
    return (jnp.cos(angle) + jnp.sin(angle)) * (count ** -0.5)


def along_dim(values, dim):
    moved = jnp.tensordot(values, basis_table(values.shape[dim]), axes=([dim], [0]), precision=lax.Precision.HIGHEST)
    return jnp.moveaxis(moved, -1, dim)


def reference(species, coupling, symbol_x, symbol_y, symbol_z):
    modes = species
    modes = along_dim(modes, 1)
    modes = along_dim(modes, 2)
    modes = along_dim(modes, 3)
    symbol = symbol_x[:, None, None] + symbol_y[None, :, None] + symbol_z[None, None, :]
    weight_xyz = 1.0 / (1.0 + symbol)
    mixed_fields = jnp.einsum("ab,bxyz->axyz", coupling, modes, precision=lax.Precision.HIGHEST)
    modes = weight_xyz * modes + (1.0 - weight_xyz) * mixed_fields
    return modes
```

```python
import jax
import jax.numpy as jnp
import numpy as np
from jax import lax
from jax.experimental import pallas as pl
from jax.experimental.pallas import tpu as pltpu
from jax.sharding import PartitionSpec as P

MESH = pl.DeviceIdType.MESH
F = 4
BLOCKS = 4

LEFT_STEPS = [(dz, dx) for dx in (0, 1, 3, 2) for dz in (1, 3, 2, 0) if (dz, dx) != (0, 0)]
RIGHT_STEPS = [(dy, dc) for dy in (1, 3, 2, 0) for dc in (0, 1) if (dy, dc) != (0, 0)]


def basis_table(count):
    rank = np.arange(count)
    angle = 2.0 * np.pi / count * (rank[:, None] * rank[None, :] % count)
    return ((np.cos(angle) + np.sin(angle)) * count**-0.5).astype(np.float32)


def halves(table):
    high = table.astype(jnp.bfloat16)
    low = (table - high.astype(np.float32)).astype(jnp.bfloat16)
    return high, low


def split(values):
    high = values.astype(jnp.bfloat16)
    return high, (values - high.astype(jnp.float32)).astype(jnp.bfloat16)


def dot_nt(a, b):
    return lax.dot_general(a, b, (((1,), (1,)), ((), ())), preferred_element_type=jnp.float32)


def dot_nn(a, b):
    return lax.dot_general(a, b, (((1,), (0,)), ((), ())), preferred_element_type=jnp.float32)


def exchange_blocks(arrays, width):
    lane = lax.broadcasted_iota(jnp.int32, arrays[0].shape, 1)
    arrays = list(arrays)
    bit = 1
    while bit < len(arrays):
        upper = (lane // width) % (2 * bit) >= bit
        for i in range(len(arrays)):
            if i & bit == 0:
                a, b = arrays[i], arrays[i + bit]
                arrays[i] = jnp.where(upper, pltpu.roll(b, width * bit, 1), a)
                arrays[i + bit] = jnp.where(upper, b, pltpu.roll(a, 128 - width * bit, 1))
        bit *= 2
    return arrays


def kernel(
    species, hx_high_hbm, hx_low_hbm, h_high_hbm, h_low_hbm, out,
    grid, hx_high, hx_low, h_high, h_low, d_high, d_low, s1, r1, d2, e_high, e_low, s2, r2, g_high, g_low, modes,
    in_sem, h_sem, send1, recv1, send2, recv2, out_sem,
):
    left, right = lax.axis_index("left"), lax.axis_index("right")
    z, x = left // 4, left % 4
    y, core = right // 2, right % 2
    left_peers = [lax.rem(z + dz, 4) * 4 + lax.rem(x + dx, 4) for dz, dx in LEFT_STEPS]
    right_peers = [lax.rem(y + dy, 4) * 2 + lax.rem(core + dc, 2) for dy, dc in RIGHT_STEPS]

    barrier = pltpu.get_barrier_semaphore()
    for peer in left_peers:
        pl.semaphore_signal(barrier, inc=1, device_id=(peer, right), device_id_type=MESH)
    for peer in right_peers:
        pl.semaphore_signal(barrier, inc=1, device_id=(left, peer), device_id_type=MESH)

    def load(f, t):
        return pltpu.make_async_copy(
            species.at[pl.ds(512 * f, 512), pl.ds(128 * t, 128)],
            grid.at[pl.ds((4 * f + t) * 512, 512)],
            in_sem.at[f, t],
        )

    for f in range(F):
        for t in range(4):
            load(f, t).start()
        if f == 0:
            tables = [
                pltpu.make_async_copy(a, b, h_sem.at[i])
                for i, (a, b) in enumerate(
                    [(hx_high_hbm, hx_high), (hx_low_hbm, hx_low), (h_high_hbm, h_high), (h_low_hbm, h_low)]
                )
            ]
            for table in tables:
                table.start()

    def first(f, b, k):
        return pltpu.make_async_remote_copy(
            src_ref=s1.at[f, b, left_peers[k]],
            dst_ref=r1.at[f, b, left],
            send_sem=send1.at[f, b],
            recv_sem=recv1.at[f, b],
            device_id=(left_peers[k], right),
            device_id_type=MESH,
        )

    def second(f, b, k):
        return pltpu.make_async_remote_copy(
            src_ref=s2.at[f, b, right_peers[k]],
            dst_ref=r2.at[f, b, right],
            send_sem=send2.at[f, b],
            recv_sem=recv2.at[f, b],
            device_id=(left, right_peers[k]),
            device_id_type=MESH,
        )

    def all_first(f, b):
        return pltpu.make_async_remote_copy(
            src_ref=s1.at[f, b, pl.ds(0, 15)],
            dst_ref=r1.at[f, b, pl.ds(0, 15)],
            send_sem=send1.at[f, b],
            recv_sem=recv1.at[f, b],
            device_id=(left_peers[0], right),
            device_id_type=MESH,
        )

    def all_second(f, b):
        return pltpu.make_async_remote_copy(
            src_ref=s2.at[f, b, pl.ds(0, 7)],
            dst_ref=r2.at[f, b, pl.ds(0, 7)],
            send_sem=send2.at[f, b],
            recv_sem=recv2.at[f, b],
            device_id=(left, right_peers[0]),
            device_id_type=MESH,
        )

    def along_x(f, opening):
        for t in range(4):
            load(f, t).wait()
        for t in range(4):
            for zi in range(32):
                rows = grid[pl.ds((4 * f + t) * 512 + zi, 16, stride=32), :]
                high, low = split(rows)
                d_high[pl.ds(16 * zi, 16), pl.ds(128 * t, 128)] = high
                d_low[pl.ds(16 * zi, 16), pl.ds(128 * t, 128)] = low
        if opening:
            for table in tables:
                table.wait()

        def block(b, carry):
            rows = pl.ds(pl.multiple_of(128 * b, 128), 128)
            part = dot_nt(hx_high[rows, :], d_high[...])
            part += dot_nt(hx_high[rows, :], d_low[...])
            part += dot_nt(hx_low[rows, :], d_high[...])
            s1[f, b] = part.reshape(16, 8, 512)
            r1[f, b, left] = s1[f, b, left]
            if opening:

                @pl.when(b == 0)
                def _():
                    pl.semaphore_wait(barrier, len(left_peers) + len(right_peers))

            for k in range(len(left_peers)):
                first(f, b, k).start()
            return carry

        lax.fori_loop(0, BLOCKS, block, 0)

    def along_y(f, b):
        all_first(f, b).wait_recv()
        for t in range(4):
            for g in range(2):
                arrays = [r1[f, b, 8 * g + i, :, pl.ds(128 * t, 128)] for i in range(8)]
                for i, array in enumerate(exchange_blocks(arrays, 16)):
                    d2[pl.ds(256 * g + 8 * (8 * t + i), 8), :] = array
        for g in range(2):
            for kx in range(8):
                high, low = split(d2[pl.ds(256 * g + kx, 32, stride=8), :])
                e_high[pl.ds(32 * kx, 32), pl.ds(128 * g, 128)] = high
                e_low[pl.ds(32 * kx, 32), pl.ds(128 * g, 128)] = low
        part = dot_nt(h_high[...], e_high[...])
        part += dot_nt(h_high[...], e_low[...])
        part += dot_nt(h_low[...], e_high[...])
        s2[f, b] = part.reshape(8, 32, 256)
        r2[f, b, right] = s2[f, b, right]
        for k in range(len(right_peers)):
            second(f, b, k).start()

    def store(f, b):
        return pltpu.make_async_copy(
            modes.at[f, pl.ds(8 * b, 8)], out.at[f, pl.ds(8 * b, 8)], out_sem.at[f, b]
        )

    def along_z(f, b):
        all_second(f, b).wait_recv()
        for t in range(2):
            for g in range(2):
                arrays = [r2[f, b, 4 * g + i, :, pl.ds(128 * t, 128)] for i in range(4)]
                for i, array in enumerate(exchange_blocks(arrays, 32)):
                    high, low = split(array)
                    g_high[pl.ds(32 * (4 * t + i), 32), pl.ds(128 * g, 128)] = high
                    g_low[pl.ds(32 * (4 * t + i), 32), pl.ds(128 * g, 128)] = low
        part = dot_nn(g_high[...], h_high[...])
        part += dot_nn(g_low[...], h_high[...])
        part += dot_nn(g_high[...], h_low[...])
        modes[f, pl.ds(8 * b, 8)] = part.reshape(8, 32, 256)
        store(f, b).start()

    along_x(0, True)

    def field(f, carry):
        @pl.when(f < F - 1)
        def _():
            along_x(f + 1, False)

        def block(b, inner):
            along_y(f, b)
            step = BLOCKS * f + b - 1

            @pl.when(step >= 0)
            def _():
                along_z(step // BLOCKS, step % BLOCKS)

            return inner

        return lax.fori_loop(0, BLOCKS, block, carry)

    lax.fori_loop(0, F, field, 0)
    along_z(F - 1, BLOCKS - 1)

    def finish(step, carry):
        f, b = step // BLOCKS, step % BLOCKS
        all_first(f, b).wait_send()
        all_second(f, b).wait_send()
        store(f, b).wait()
        return carry

    lax.fori_loop(0, F * BLOCKS, finish, 0)


def transform(species):
    any_space = pl.BlockSpec(memory_space=pl.ANY)
    wide = basis_table(512)
    rows = np.arange(512).reshape(16, BLOCKS, 8).transpose(1, 0, 2).reshape(-1)
    hx_high, hx_low = halves(wide[rows])
    h_high, h_low = halves(basis_table(256))
    flat = jnp.transpose(species, (0, 2, 3, 1)).reshape(F * 512, 512)
    return pl.pallas_call(
        kernel,
        out_shape=jax.ShapeDtypeStruct((F, 32, 32, 256), jnp.float32),
        in_specs=[any_space] * 5,
        out_specs=any_space,
        scratch_shapes=[
            pltpu.VMEM((F * 4 * 512, 128), jnp.float32),
            pltpu.VMEM((512, 512), jnp.bfloat16),
            pltpu.VMEM((512, 512), jnp.bfloat16),
            pltpu.VMEM((256, 256), jnp.bfloat16),
            pltpu.VMEM((256, 256), jnp.bfloat16),
            pltpu.VMEM((512, 512), jnp.bfloat16),
            pltpu.VMEM((512, 512), jnp.bfloat16),
            pltpu.VMEM((F, BLOCKS, 16, 8, 512), jnp.float32),
            pltpu.VMEM((F, BLOCKS, 16, 8, 512), jnp.float32),
            pltpu.VMEM((512, 128), jnp.float32),
            pltpu.VMEM((256, 256), jnp.bfloat16),
            pltpu.VMEM((256, 256), jnp.bfloat16),
            pltpu.VMEM((F, BLOCKS, 8, 32, 256), jnp.float32),
            pltpu.VMEM((F, BLOCKS, 8, 32, 256), jnp.float32),
            pltpu.VMEM((256, 256), jnp.bfloat16),
            pltpu.VMEM((256, 256), jnp.bfloat16),
            pltpu.VMEM((F, 32, 32, 256), jnp.float32),
            pltpu.SemaphoreType.DMA((F, 4)),
            pltpu.SemaphoreType.DMA((4,)),
            pltpu.SemaphoreType.DMA((F, BLOCKS)),
            pltpu.SemaphoreType.DMA((F, BLOCKS)),
            pltpu.SemaphoreType.DMA((F, BLOCKS)),
            pltpu.SemaphoreType.DMA((F, BLOCKS)),
            pltpu.SemaphoreType.DMA((F, BLOCKS)),
        ],
        compiler_params=pltpu.CompilerParams(
            collective_id=0, has_side_effects=True, vmem_limit_bytes=48 * 2**20
        ),
        name="transform",
    )(flat, hx_high, hx_low, h_high, h_low)


def body(species, coupling, symbol_x, symbol_y, symbol_z):
    modes = transform(species)
    part_x = lax.dynamic_slice_in_dim(symbol_x, lax.axis_index("left") * 32, 32)
    part_y = lax.dynamic_slice_in_dim(symbol_y, lax.axis_index("right") * 32, 32)
    symbol = part_x[:, None, None] + part_y[None, :, None] + symbol_z[None, None, :]
    weight = 1.0 / (1.0 + symbol)
    fields = []
    for a in range(F):
        mixed = sum(coupling[a, b] * modes[b] for b in range(F))
        fields.append(weight * modes[a] + (1.0 - weight) * mixed)
    return jnp.stack(fields)


def solution(mesh):
    in_specs = (P(None, None, "left", "right"), P(), P(), P(), P())
    out_specs = P(None, "left", "right", None)
    return jax.shard_map(body, mesh=mesh, in_specs=in_specs, out_specs=out_specs, check_vma=False)
```

```python
import jax
import jax.numpy as jnp
import numpy as np
from jax import lax
from jax.experimental import pallas as pl
from jax.experimental.pallas import tpu as pltpu
from jax.sharding import PartitionSpec as P

MESH = pl.DeviceIdType.MESH
F = 4
BLOCKS = 4
LAG = 2

LEFT_STEPS = [(dz, dx) for dx in (0, 1, 3, 2) for dz in (1, 3, 2, 0) if (dz, dx) != (0, 0)]
RIGHT_STEPS = [(dy, dc) for dy in (1, 3, 2, 0) for dc in (0, 1) if (dy, dc) != (0, 0)]


def basis_table(count):
    rank = np.arange(count)
    angle = 2.0 * np.pi / count * (rank[:, None] * rank[None, :] % count)
    return ((np.cos(angle) + np.sin(angle)) * count**-0.5).astype(np.float32)


def halves(table):
    high = table.astype(jnp.bfloat16)
    low = (table - high.astype(np.float32)).astype(jnp.bfloat16)
    return high, low


def split(values):
    high = values.astype(jnp.bfloat16)
    return high, (values - high.astype(jnp.float32)).astype(jnp.bfloat16)


def dot_nt(a, b):
    return lax.dot_general(a, b, (((1,), (1,)), ((), ())), preferred_element_type=jnp.float32)


def dot_nn(a, b):
    return lax.dot_general(a, b, (((1,), (0,)), ((), ())), preferred_element_type=jnp.float32)


def exchange_blocks(arrays, width):
    lane = lax.broadcasted_iota(jnp.int32, arrays[0].shape, 1)
    arrays = list(arrays)
    bit = 1
    while bit < len(arrays):
        upper = (lane // width) % (2 * bit) >= bit
        for i in range(len(arrays)):
            if i & bit == 0:
                a, b = arrays[i], arrays[i + bit]
                arrays[i] = jnp.where(upper, pltpu.roll(b, width * bit, 1), a)
                arrays[i + bit] = jnp.where(upper, b, pltpu.roll(a, 128 - width * bit, 1))
        bit *= 2
    return arrays


def kernel(
    species, tables_x, tables, coupling, symbol_x, symbol_y, symbol_z, out,
    grid, hx, h, d_high, d_low, s1, r1, d2, e_high, e_low, s2, r2, g_high, g_low, modes, base, mix, sx, sy, sz,
    in_sem, h_sem, send1, recv1, send2, recv2,
):
    left, right = lax.axis_index("left"), lax.axis_index("right")
    z, x = left // 4, left % 4
    y, core = right // 2, right % 2
    left_peers = [lax.rem(z + dz, 4) * 4 + lax.rem(x + dx, 4) for dz, dx in LEFT_STEPS]
    right_peers = [lax.rem(y + dy, 4) * 2 + lax.rem(core + dc, 2) for dy, dc in RIGHT_STEPS]

    def load(f, t):
        return pltpu.make_async_copy(
            species.at[pl.ds(512 * f, 512), pl.ds(128 * t, 128)],
            grid.at[pl.ds((4 * f + t) * 512, 512)],
            in_sem.at[f, t],
        )

    small = [
        pltpu.make_async_copy(a, b, h_sem.at[i])
        for i, (a, b) in enumerate(
            [(tables_x, hx), (tables, h), (coupling, mix), (symbol_x, sx), (symbol_y, sy), (symbol_z, sz)]
        )
    ]
    for t in range(4):
        load(0, t).start()
    small[0].start()
    for f in range(1, F):
        for t in range(4):
            load(f, t).start()
    for copy in small[1:]:
        copy.start()

    barrier = pltpu.get_barrier_semaphore()
    for peer in left_peers:
        pl.semaphore_signal(barrier, inc=1, device_id=(peer, right), device_id_type=MESH)
    for peer in right_peers:
        pl.semaphore_signal(barrier, inc=1, device_id=(left, peer), device_id_type=MESH)

    def first(f, b, k):
        return pltpu.make_async_remote_copy(
            src_ref=s1.at[f, b, left_peers[k]],
            dst_ref=r1.at[f, b, left],
            send_sem=send1.at[f, b],
            recv_sem=recv1.at[f, b],
            device_id=(left_peers[k], right),
            device_id_type=MESH,
        )

    def second(f, b, k):
        return pltpu.make_async_remote_copy(
            src_ref=s2.at[f, b, right_peers[k]],
            dst_ref=r2.at[f, b, right],
            send_sem=send2.at[f, b],
            recv_sem=recv2.at[f, b],
            device_id=(left, right_peers[k]),
            device_id_type=MESH,
        )

    def all_first(f, b):
        return pltpu.make_async_remote_copy(
            src_ref=s1.at[f, b, pl.ds(0, 15)],
            dst_ref=r1.at[f, b, pl.ds(0, 15)],
            send_sem=send1.at[f, b],
            recv_sem=recv1.at[f, b],
            device_id=(left_peers[0], right),
            device_id_type=MESH,
        )

    def all_second(f, b):
        return pltpu.make_async_remote_copy(
            src_ref=s2.at[f, b, pl.ds(0, 7)],
            dst_ref=r2.at[f, b, pl.ds(0, 7)],
            send_sem=send2.at[f, b],
            recv_sem=recv2.at[f, b],
            device_id=(left, right_peers[0]),
            device_id_type=MESH,
        )

    def send_first(f, b):
        for k in range(len(left_peers)):
            first(f, b, k).start()

    def along_x(f, carry):
        for t in range(4):
            load(f, t).wait()
        for t in range(4):
            for zi in range(32):
                rows = grid[pl.ds((4 * f + t) * 512 + zi, 16, stride=32), :]
                high, low = split(rows)
                d_high[pl.ds(16 * zi, 16), pl.ds(128 * t, 128)] = high
                d_low[pl.ds(16 * zi, 16), pl.ds(128 * t, 128)] = low

        @pl.when(f == 0)
        def _():
            small[0].wait()

        def pair(p, inner):
            rows = pl.ds(pl.multiple_of(256 * p, 256), 256)
            part = dot_nt(hx[0, rows, :], d_high[...])
            part += dot_nt(hx[0, rows, :], d_low[...])
            part += dot_nt(hx[1, rows, :], d_high[...])
            s1[f, pl.ds(2 * p, 2)] = part.reshape(2, 16, 8, 512)
            for i in range(2):
                r1[f, 2 * p + i, left] = s1[f, 2 * p + i, left]

            @pl.when(p == 0)
            def _():
                @pl.when(f == 0)
                def _():
                    pl.semaphore_wait(barrier, len(left_peers) + len(right_peers))

                send_first(f, 0)

            return inner

        return lax.fori_loop(0, BLOCKS // 2, pair, carry)

    def along_y(f, b):
        all_first(f, b).wait_recv()
        for t in range(4):
            for g in range(2):
                arrays = [r1[f, b, 8 * g + i, :, pl.ds(128 * t, 128)] for i in range(8)]
                for i, array in enumerate(exchange_blocks(arrays, 16)):
                    d2[pl.ds(256 * g + 8 * (8 * t + i), 8), :] = array
        for g in range(2):
            for kx in range(8):
                high, low = split(d2[pl.ds(256 * g + kx, 32, stride=8), :])
                e_high[pl.ds(32 * kx, 32), pl.ds(128 * g, 128)] = high
                e_low[pl.ds(32 * kx, 32), pl.ds(128 * g, 128)] = low
        part = dot_nt(h[0], e_high[...])
        part += dot_nt(h[0], e_low[...])
        part += dot_nt(h[1], e_high[...])
        s2[f, b] = part.reshape(8, 32, 256)
        r2[f, b, right] = s2[f, b, right]
        for k in range(len(right_peers)):
            second(f, b, k).start()

    def along_z(f, b):
        all_second(f, b).wait_recv()
        for t in range(2):
            for g in range(2):
                arrays = [r2[f, b, 4 * g + i, :, pl.ds(128 * t, 128)] for i in range(4)]
                for i, array in enumerate(exchange_blocks(arrays, 32)):
                    high, low = split(array)
                    g_high[pl.ds(32 * (4 * t + i), 32), pl.ds(128 * g, 128)] = high
                    g_low[pl.ds(32 * (4 * t + i), 32), pl.ds(128 * g, 128)] = low
        part = dot_nn(g_high[...], h[0])
        part += dot_nn(g_low[...], h[0])
        part += dot_nn(g_high[...], h[1])
        modes[f] = part.reshape(8, 32, 256)

    def mixing(b):
        weights = [[mix[a, c] for c in range(F)] for a in range(F)]

        def plane(kx, carry):
            shift = sx[32 * left + 8 * b + kx]
            for part in range(4):
                rows = pl.ds(8 * part, 8)
                weight = 1.0 / (base[rows, :] + shift)
                other = 1.0 - weight
                old = [modes[a, kx, rows, :] for a in range(F)]
                for a in range(F):
                    mixed = weights[a][0] * old[0]
                    for c in range(1, F):
                        mixed += weights[a][c] * old[c]
                    out[a, 8 * b + kx, rows, :] = weight * old[a] + other * mixed
            return carry

        lax.fori_loop(0, 8, plane, 0)

    lax.fori_loop(0, F, along_x, 0)

    def send_rest(step, carry):
        send_first(step % F, step // F)
        return carry

    lax.fori_loop(F, F * BLOCKS, send_rest, 0)
    for copy in small[1:]:
        copy.wait()
    for ky in range(32):
        base[pl.ds(ky, 1), :] = 1.0 + (sz[...] + sy[32 * right + ky])

    def step(i, carry):
        @pl.when(i < F * BLOCKS)
        def _():
            along_y(i % F, i // F)

        @pl.when(i >= LAG)
        def _():
            j = i - LAG
            along_z(j % F, j // F)

            @pl.when(j % F == F - 1)
            def _():
                mixing(j // F)

        return carry

    lax.fori_loop(0, F * BLOCKS + LAG, step, 0)

    def finish(i, carry):
        all_first(i % F, i // F).wait_send()
        all_second(i % F, i // F).wait_send()
        return carry

    lax.fori_loop(0, F * BLOCKS, finish, 0)


def body(species, coupling, symbol_x, symbol_y, symbol_z):
    hbm = pl.BlockSpec(memory_space=pltpu.HBM)
    wide = basis_table(512)
    rows = np.arange(512).reshape(16, BLOCKS, 8).transpose(1, 0, 2).reshape(-1)
    tables_x = np.stack(halves(wide[rows]))
    tables = np.stack(halves(basis_table(256)))
    flat = jnp.transpose(species, (0, 2, 3, 1)).reshape(F * 512, 512)
    arrays = (flat, tables_x, tables, coupling, symbol_x, symbol_y, symbol_z.reshape(1, 256))
    return pl.pallas_call(
        kernel,
        out_shape=jax.ShapeDtypeStruct((F, 32, 32, 256), jnp.float32),
        in_specs=[hbm] * 7,
        out_specs=pl.BlockSpec(memory_space=pltpu.VMEM),
        scratch_shapes=[
            pltpu.VMEM((F * 4 * 512, 128), jnp.float32),
            pltpu.VMEM((2, 512, 512), jnp.bfloat16),
            pltpu.VMEM((2, 256, 256), jnp.bfloat16),
            pltpu.VMEM((512, 512), jnp.bfloat16),
            pltpu.VMEM((512, 512), jnp.bfloat16),
            pltpu.VMEM((F, BLOCKS, 16, 8, 512), jnp.float32),
            pltpu.VMEM((F, BLOCKS, 16, 8, 512), jnp.float32),
            pltpu.VMEM((512, 128), jnp.float32),
            pltpu.VMEM((256, 256), jnp.bfloat16),
            pltpu.VMEM((256, 256), jnp.bfloat16),
            pltpu.VMEM((F, BLOCKS, 8, 32, 256), jnp.float32),
            pltpu.VMEM((F, BLOCKS, 8, 32, 256), jnp.float32),
            pltpu.VMEM((256, 256), jnp.bfloat16),
            pltpu.VMEM((256, 256), jnp.bfloat16),
            pltpu.VMEM((F, 8, 32, 256), jnp.float32),
            pltpu.VMEM((32, 256), jnp.float32),
            pltpu.SMEM((F, F), jnp.float32),
            pltpu.SMEM((512,), jnp.float32),
            pltpu.SMEM((256,), jnp.float32),
            pltpu.VMEM((1, 256), jnp.float32),
            pltpu.SemaphoreType.DMA((F, 4)),
            pltpu.SemaphoreType.DMA((6,)),
            pltpu.SemaphoreType.DMA((F, BLOCKS)),
            pltpu.SemaphoreType.DMA((F, BLOCKS)),
            pltpu.SemaphoreType.DMA((F, BLOCKS)),
            pltpu.SemaphoreType.DMA((F, BLOCKS)),
        ],
        compiler_params=pltpu.CompilerParams(
            collective_id=0, has_side_effects=True, vmem_limit_bytes=40 * 2**20
        ),
        name="transform",
    )(*(pltpu.with_memory_space_constraint(a, pltpu.HBM) for a in arrays))


def solution(mesh):
    in_specs = (P(None, None, "left", "right"), P(), P(), P(), P())
    out_specs = P(None, "left", "right", None)
    return jax.shard_map(body, mesh=mesh, in_specs=in_specs, out_specs=out_specs, check_vma=False)
```

```python
import jax
import jax.numpy as jnp
import numpy as np
from jax import lax
from jax.experimental import pallas as pl
from jax.experimental.pallas import tpu as pltpu
from jax.sharding import PartitionSpec as P

MESH = pl.DeviceIdType.MESH
F = 4
BLOCKS = 4
LAG = 3
AHEAD = 8

LEFT_STEPS = [(dz, dx) for dx in (2, 1, 3, 0) for dz in (2, 1, 3, 0) if (dz, dx) != (0, 0)]
RIGHT_STEPS = [(dy, dc) for dy in (2, 1, 3, 0) for dc in (0, 1) if (dy, dc) != (0, 0)]


def basis_table(count):
    rank = np.arange(count)
    angle = 2.0 * np.pi / count * (rank[:, None] * rank[None, :] % count)
    return ((np.cos(angle) + np.sin(angle)) * count**-0.5).astype(np.float32)


def halves(table):
    high = table.astype(jnp.bfloat16)
    low = (table - high.astype(np.float32)).astype(jnp.bfloat16)
    return high, low


def split(values):
    high = values.astype(jnp.bfloat16)
    return high, (values - high.astype(jnp.float32)).astype(jnp.bfloat16)


def dot_nt(a, b):
    return lax.dot_general(a, b, (((1,), (1,)), ((), ())), preferred_element_type=jnp.float32)


def dot_nn(a, b):
    return lax.dot_general(a, b, (((1,), (0,)), ((), ())), preferred_element_type=jnp.float32)


def exchange_blocks(arrays, width):
    lane = lax.broadcasted_iota(jnp.int32, arrays[0].shape, 1)
    arrays = list(arrays)
    bit = 1
    while bit < len(arrays):
        upper = (lane // width) % (2 * bit) >= bit
        for i in range(len(arrays)):
            if i & bit == 0:
                a, b = arrays[i], arrays[i + bit]
                arrays[i] = jnp.where(upper, pltpu.roll(b, width * bit, 1), a)
                arrays[i + bit] = jnp.where(upper, b, pltpu.roll(a, 128 - width * bit, 1))
        bit *= 2
    return arrays


def kernel(
    species, tables_x, tables, coupling, symbol_x, symbol_y, symbol_z, out,
    grid, hx, h, d_high, d_low, s1, r1, d2, e_high, e_low, s2, r2, g_high, g_low, modes, base, mix, sx, sy, sz,
    in_sem, h_sem, send1, recv1, send2, recv2,
):
    left, right = lax.axis_index("left"), lax.axis_index("right")
    z, x = left // 4, left % 4
    y, core = right // 2, right % 2
    left_peers = [lax.rem(z + dz, 4) * 4 + lax.rem(x + dx, 4) for dz, dx in LEFT_STEPS]
    right_peers = [lax.rem(y + dy, 4) * 2 + lax.rem(core + dc, 2) for dy, dc in RIGHT_STEPS]

    def load(f, t):
        return pltpu.make_async_copy(
            species.at[pl.ds(512 * f, 512), pl.ds(128 * t, 128)],
            grid.at[pl.ds((4 * f + t) * 512, 512)],
            in_sem.at[f, t],
        )

    small = [
        pltpu.make_async_copy(a, b, h_sem.at[i])
        for i, (a, b) in enumerate(
            [(tables_x, hx), (tables, h), (coupling, mix), (symbol_x, sx), (symbol_y, sy), (symbol_z, sz)]
        )
    ]
    for t in range(4):
        load(0, t).start()
    small[0].start()
    for f in range(1, F):
        for t in range(4):
            load(f, t).start()
    for copy in small[1:]:
        copy.start()

    barrier = pltpu.get_barrier_semaphore()
    for peer in left_peers:
        pl.semaphore_signal(barrier, inc=1, device_id=(peer, right), device_id_type=MESH)
    for peer in right_peers:
        pl.semaphore_signal(barrier, inc=1, device_id=(left, peer), device_id_type=MESH)

    def first(f, b, k):
        return pltpu.make_async_remote_copy(
            src_ref=s1.at[f, b, left_peers[k]],
            dst_ref=r1.at[f, b, left],
            send_sem=send1.at[f, b],
            recv_sem=recv1.at[f, b],
            device_id=(left_peers[k], right),
            device_id_type=MESH,
        )

    def second(f, b, k):
        return pltpu.make_async_remote_copy(
            src_ref=s2.at[f, b, right_peers[k]],
            dst_ref=r2.at[f, b, right],
            send_sem=send2.at[f, b],
            recv_sem=recv2.at[f, b],
            device_id=(left, right_peers[k]),
            device_id_type=MESH,
        )

    def all_first(f, b):
        return pltpu.make_async_remote_copy(
            src_ref=s1.at[f, b, pl.ds(0, 15)],
            dst_ref=r1.at[f, b, pl.ds(0, 15)],
            send_sem=send1.at[f, b],
            recv_sem=recv1.at[f, b],
            device_id=(left_peers[0], right),
            device_id_type=MESH,
        )

    def all_second(f, b):
        return pltpu.make_async_remote_copy(
            src_ref=s2.at[f, b, pl.ds(0, 7)],
            dst_ref=r2.at[f, b, pl.ds(0, 7)],
            send_sem=send2.at[f, b],
            recv_sem=recv2.at[f, b],
            device_id=(left, right_peers[0]),
            device_id_type=MESH,
        )

    def send_first(f, b):
        for k in range(len(left_peers)):
            first(f, b, k).start()

    def arrange(f):
        for t in range(4):
            load(f, t).wait()
        for t in range(4):
            for zi in range(32):
                rows = grid[pl.ds((4 * f + t) * 512 + zi, 16, stride=32), :]
                high, low = split(rows)
                d_high[f, pl.ds(16 * zi, 16), pl.ds(128 * t, 128)] = high
                d_low[f, pl.ds(16 * zi, 16), pl.ds(128 * t, 128)] = low

    def along_x(f, p):
        rows = pl.ds(pl.multiple_of(256 * p, 256), 256)
        part = dot_nt(hx[0, rows, :], d_high[f])
        part += dot_nt(hx[0, rows, :], d_low[f])
        part += dot_nt(hx[1, rows, :], d_high[f])
        s1[f, pl.ds(2 * p, 2)] = part.reshape(2, 16, 8, 512)
        for i in range(2):
            r1[f, 2 * p + i, left] = s1[f, 2 * p + i, left]

    def opening(f, carry):
        arrange(f)

        @pl.when(f == 0)
        def _():
            small[0].wait()

        along_x(f, 0)

        @pl.when(f == 0)
        def _():
            pl.semaphore_wait(barrier, len(left_peers) + len(right_peers))

        send_first(f, 0)
        return carry

    def along_y(f, b):
        all_first(f, b).wait_recv()
        for t in range(4):
            for g in range(2):
                arrays = [r1[f, b, 8 * g + i, :, pl.ds(128 * t, 128)] for i in range(8)]
                for i, array in enumerate(exchange_blocks(arrays, 16)):
                    d2[pl.ds(256 * g + 8 * (8 * t + i), 8), :] = array
        for g in range(2):
            for kx in range(8):
                high, low = split(d2[pl.ds(256 * g + kx, 32, stride=8), :])
                e_high[pl.ds(32 * kx, 32), pl.ds(128 * g, 128)] = high
                e_low[pl.ds(32 * kx, 32), pl.ds(128 * g, 128)] = low
        part = dot_nt(h[0], e_high[...])
        part += dot_nt(h[0], e_low[...])
        part += dot_nt(h[1], e_high[...])
        s2[f, b] = part.reshape(8, 32, 256)
        r2[f, b, right] = s2[f, b, right]
        for k in range(len(right_peers)):
            second(f, b, k).start()

    def along_z(f, b):
        all_second(f, b).wait_recv()
        for t in range(2):
            for g in range(2):
                arrays = [r2[f, b, 4 * g + i, :, pl.ds(128 * t, 128)] for i in range(4)]
                for i, array in enumerate(exchange_blocks(arrays, 32)):
                    high, low = split(array)
                    g_high[pl.ds(32 * (4 * t + i), 32), pl.ds(128 * g, 128)] = high
                    g_low[pl.ds(32 * (4 * t + i), 32), pl.ds(128 * g, 128)] = low
        part = dot_nn(g_high[...], h[0])
        part += dot_nn(g_low[...], h[0])
        part += dot_nn(g_high[...], h[1])
        modes[f] = part.reshape(8, 32, 256)

    def mixing(b):
        weights = [[mix[a, c] for c in range(F)] for a in range(F)]

        def plane(kx, carry):
            shift = sx[32 * left + 8 * b + kx]
            for part in range(4):
                rows = pl.ds(8 * part, 8)
                weight = 1.0 / (base[rows, :] + shift)
                other = 1.0 - weight
                old = [modes[a, kx, rows, :] for a in range(F)]
                for a in range(F):
                    mixed = weights[a][0] * old[0]
                    for c in range(1, F):
                        mixed += weights[a][c] * old[c]
                    out[a, 8 * b + kx, rows, :] = weight * old[a] + other * mixed
            return carry

        lax.fori_loop(0, 8, plane, 0)

    lax.fori_loop(0, F, opening, 0)

    def send_chunk(c, carry):
        send_first(c % F, c // F)
        return carry

    lax.fori_loop(F, AHEAD, send_chunk, 0)
    small[1].wait()

    def step(i, carry):
        @pl.when(i < F * BLOCKS)
        def _():
            along_y(i % F, i // F)

        @pl.when(i >= LAG)
        def _():
            j = i - LAG
            along_z(j % F, j // F)

            @pl.when(j % F == F - 1)
            def _():
                mixing(j // F)

        @pl.when(i < F)
        def _():
            along_x(i, 1)

        @pl.when(i + AHEAD < F * BLOCKS)
        def _():
            send_chunk(i + AHEAD, 0)

        @pl.when(i == F)
        def _():
            for copy in small[2:]:
                copy.wait()
            for ky in range(32):
                base[pl.ds(ky, 1), :] = 1.0 + (sz[...] + sy[32 * right + ky])

        return carry

    lax.fori_loop(0, F * BLOCKS + LAG, step, 0)

    def finish(i, carry):
        all_first(i % F, i // F).wait_send()
        all_second(i % F, i // F).wait_send()
        return carry

    lax.fori_loop(0, F * BLOCKS, finish, 0)


def body(species, coupling, symbol_x, symbol_y, symbol_z):
    hbm = pl.BlockSpec(memory_space=pltpu.HBM)
    wide = basis_table(512)
    rows = np.arange(512).reshape(16, BLOCKS, 8).transpose(1, 0, 2).reshape(-1)
    tables_x = np.stack(halves(wide[rows]))
    tables = np.stack(halves(basis_table(256)))
    flat = jnp.transpose(species, (0, 2, 3, 1)).reshape(F * 512, 512)
    arrays = (flat, tables_x, tables, coupling, symbol_x, symbol_y, symbol_z.reshape(1, 256))
    return pl.pallas_call(
        kernel,
        out_shape=jax.ShapeDtypeStruct((F, 32, 32, 256), jnp.float32),
        in_specs=[hbm] * 7,
        out_specs=pl.BlockSpec(memory_space=pltpu.VMEM),
        scratch_shapes=[
            pltpu.VMEM((F * 4 * 512, 128), jnp.float32),
            pltpu.VMEM((2, 512, 512), jnp.bfloat16),
            pltpu.VMEM((2, 256, 256), jnp.bfloat16),
            pltpu.VMEM((F, 512, 512), jnp.bfloat16),
            pltpu.VMEM((F, 512, 512), jnp.bfloat16),
            pltpu.VMEM((F, BLOCKS, 16, 8, 512), jnp.float32),
            pltpu.VMEM((F, BLOCKS, 16, 8, 512), jnp.float32),
            pltpu.VMEM((512, 128), jnp.float32),
            pltpu.VMEM((256, 256), jnp.bfloat16),
            pltpu.VMEM((256, 256), jnp.bfloat16),
            pltpu.VMEM((F, BLOCKS, 8, 32, 256), jnp.float32),
            pltpu.VMEM((F, BLOCKS, 8, 32, 256), jnp.float32),
            pltpu.VMEM((256, 256), jnp.bfloat16),
            pltpu.VMEM((256, 256), jnp.bfloat16),
            pltpu.VMEM((F, 8, 32, 256), jnp.float32),
            pltpu.VMEM((32, 256), jnp.float32),
            pltpu.SMEM((F, F), jnp.float32),
            pltpu.SMEM((512,), jnp.float32),
            pltpu.SMEM((256,), jnp.float32),
            pltpu.VMEM((1, 256), jnp.float32),
            pltpu.SemaphoreType.DMA((F, 4)),
            pltpu.SemaphoreType.DMA((6,)),
            pltpu.SemaphoreType.DMA((F, BLOCKS)),
            pltpu.SemaphoreType.DMA((F, BLOCKS)),
            pltpu.SemaphoreType.DMA((F, BLOCKS)),
            pltpu.SemaphoreType.DMA((F, BLOCKS)),
        ],
        compiler_params=pltpu.CompilerParams(
            collective_id=0, has_side_effects=True, vmem_limit_bytes=40 * 2**20
        ),
        name="transform",
    )(*(pltpu.with_memory_space_constraint(a, pltpu.HBM) for a in arrays))


def solution(mesh):
    in_specs = (P(None, None, "left", "right"), P(), P(), P(), P())
    out_specs = P(None, "left", "right", None)
    return jax.shard_map(body, mesh=mesh, in_specs=in_specs, out_specs=out_specs, check_vma=False)
```

```python
import jax
import jax.numpy as jnp
import numpy as np
from jax import lax
from jax.experimental import pallas as pl
from jax.experimental.pallas import tpu as pltpu
from jax.sharding import PartitionSpec as P

MESH = pl.DeviceIdType.MESH
F = 4
BLOCKS = 4
LAG = 3
AHEAD = 8
LAST = F * BLOCKS - 1

LEFT_STEPS = [(dz, dx) for dx in (2, 1, 3, 0) for dz in (2, 1, 3, 0) if (dz, dx) != (0, 0)]
RIGHT_STEPS = [(dy, dc) for dy in (2, 1, 3, 0) for dc in (0, 1) if (dy, dc) != (0, 0)]


def basis_table(count):
    rank = np.arange(count)
    angle = 2.0 * np.pi / count * (rank[:, None] * rank[None, :] % count)
    return ((np.cos(angle) + np.sin(angle)) * count**-0.5).astype(np.float32)


def halves(table):
    high = table.astype(jnp.bfloat16)
    low = (table - high.astype(np.float32)).astype(jnp.bfloat16)
    return high, low


def split(values):
    high = values.astype(jnp.bfloat16)
    return high, (values - high.astype(jnp.float32)).astype(jnp.bfloat16)


def dot_nt(a, b):
    return lax.dot_general(a, b, (((1,), (1,)), ((), ())), preferred_element_type=jnp.float32)


def dot_nn(a, b):
    return lax.dot_general(a, b, (((1,), (0,)), ((), ())), preferred_element_type=jnp.float32)


def exchange_blocks(arrays, width):
    lane = lax.broadcasted_iota(jnp.int32, arrays[0].shape, 1)
    arrays = list(arrays)
    bit = 1
    while bit < len(arrays):
        upper = (lane // width) % (2 * bit) >= bit
        for i in range(len(arrays)):
            if i & bit == 0:
                a, b = arrays[i], arrays[i + bit]
                arrays[i] = jnp.where(upper, pltpu.roll(b, width * bit, 1), a)
                arrays[i + bit] = jnp.where(upper, b, pltpu.roll(a, 128 - width * bit, 1))
        bit *= 2
    return arrays


def z_transform(pieces, h, g_high, g_low):
    for t in range(2):
        for g in range(2):
            arrays = [pieces[4 * g + i, :, pl.ds(128 * t, 128)] for i in range(4)]
            for i, array in enumerate(exchange_blocks(arrays, 32)):
                high, low = split(array)
                g_high[pl.ds(32 * (4 * t + i), 32), pl.ds(128 * g, 128)] = high
                g_low[pl.ds(32 * (4 * t + i), 32), pl.ds(128 * g, 128)] = low
    part = dot_nn(g_high[...], h[0])
    part += dot_nn(g_low[...], h[0])
    part += dot_nn(g_high[...], h[1])
    return part.reshape(8, 32, 256)


def kernel(
    species, tables_x, tables, coupling, symbol_x, symbol_y, symbol_z, out, h, partial, slope, tail,
    grid, hx, d_high, d_low, s1, r1, d2, e_high, e_low, s2, r2, g_high, g_low, modes, base, mix, sx, sy, sz,
    in_sem, h_sem, send1, recv1, send2, recv2,
):
    left, right = lax.axis_index("left"), lax.axis_index("right")
    z, x = left // 4, left % 4
    y, core = right // 2, right % 2
    left_peers = [lax.rem(z + dz, 4) * 4 + lax.rem(x + dx, 4) for dz, dx in LEFT_STEPS]
    right_peers = [lax.rem(y + dy, 4) * 2 + lax.rem(core + dc, 2) for dy, dc in RIGHT_STEPS]

    def load(f, t):
        return pltpu.make_async_copy(
            species.at[pl.ds(512 * f, 512), pl.ds(128 * t, 128)],
            grid.at[pl.ds((4 * f + t) * 512, 512)],
            in_sem.at[f, t],
        )

    small = [
        pltpu.make_async_copy(a, b, h_sem.at[i])
        for i, (a, b) in enumerate(
            [(tables_x, hx), (tables, h), (coupling, mix), (symbol_x, sx), (symbol_y, sy), (symbol_z, sz)]
        )
    ]
    for t in range(4):
        load(0, t).start()
    small[0].start()
    for f in range(1, F):
        for t in range(4):
            load(f, t).start()
    for copy in small[1:]:
        copy.start()

    barrier = pltpu.get_barrier_semaphore()
    for peer in left_peers:
        pl.semaphore_signal(barrier, inc=1, device_id=(peer, right), device_id_type=MESH)
    for peer in right_peers:
        pl.semaphore_signal(barrier, inc=1, device_id=(left, peer), device_id_type=MESH)

    def first(f, b, k):
        return pltpu.make_async_remote_copy(
            src_ref=s1.at[f, b, left_peers[k]],
            dst_ref=r1.at[f, b, left],
            send_sem=send1.at[f, b],
            recv_sem=recv1.at[f, b],
            device_id=(left_peers[k], right),
            device_id_type=MESH,
        )

    def second(f, b, k):
        return pltpu.make_async_remote_copy(
            src_ref=s2.at[f, b, right_peers[k]],
            dst_ref=r2.at[f, b, right],
            send_sem=send2.at[f, b],
            recv_sem=recv2.at[f, b],
            device_id=(left, right_peers[k]),
            device_id_type=MESH,
        )

    def all_first(f, b):
        return pltpu.make_async_remote_copy(
            src_ref=s1.at[f, b, pl.ds(0, 15)],
            dst_ref=r1.at[f, b, pl.ds(0, 15)],
            send_sem=send1.at[f, b],
            recv_sem=recv1.at[f, b],
            device_id=(left_peers[0], right),
            device_id_type=MESH,
        )

    def all_second(f, b):
        return pltpu.make_async_remote_copy(
            src_ref=s2.at[f, b, pl.ds(0, 7)],
            dst_ref=r2.at[f, b, pl.ds(0, 7)],
            send_sem=send2.at[f, b],
            recv_sem=recv2.at[f, b],
            device_id=(left, right_peers[0]),
            device_id_type=MESH,
        )

    def send_first(f, b):
        for k in range(len(left_peers)):
            first(f, b, k).start()

    def arrange(f):
        for t in range(4):
            load(f, t).wait()
        for t in range(4):
            for zi in range(32):
                rows = grid[pl.ds((4 * f + t) * 512 + zi, 16, stride=32), :]
                high, low = split(rows)
                d_high[f, pl.ds(16 * zi, 16), pl.ds(128 * t, 128)] = high
                d_low[f, pl.ds(16 * zi, 16), pl.ds(128 * t, 128)] = low

    def along_x(f, p):
        rows = pl.ds(pl.multiple_of(256 * p, 256), 256)
        part = dot_nt(hx[0, rows, :], d_high[f])
        part += dot_nt(hx[0, rows, :], d_low[f])
        part += dot_nt(hx[1, rows, :], d_high[f])
        s1[f, pl.ds(2 * p, 2)] = part.reshape(2, 16, 8, 512)
        for i in range(2):
            r1[f, 2 * p + i, left] = s1[f, 2 * p + i, left]

    def opening(f, carry):
        arrange(f)

        @pl.when(f == 0)
        def _():
            small[0].wait()

        along_x(f, 0)

        @pl.when(f == 0)
        def _():
            pl.semaphore_wait(barrier, len(left_peers) + len(right_peers))

        send_first(f, 0)
        return carry

    def along_y(f, b):
        all_first(f, b).wait_recv()
        for t in range(4):
            for g in range(2):
                arrays = [r1[f, b, 8 * g + i, :, pl.ds(128 * t, 128)] for i in range(8)]
                for i, array in enumerate(exchange_blocks(arrays, 16)):
                    d2[pl.ds(256 * g + 8 * (8 * t + i), 8), :] = array
        for g in range(2):
            for kx in range(8):
                high, low = split(d2[pl.ds(256 * g + kx, 32, stride=8), :])
                e_high[pl.ds(32 * kx, 32), pl.ds(128 * g, 128)] = high
                e_low[pl.ds(32 * kx, 32), pl.ds(128 * g, 128)] = low
        part = dot_nt(h[0], e_high[...])
        part += dot_nt(h[0], e_low[...])
        part += dot_nt(h[1], e_high[...])
        s2[f, b] = part.reshape(8, 32, 256)
        r2[f, b, right] = s2[f, b, right]
        for k in range(len(right_peers)):
            second(f, b, k).start()

    def along_z(f, b):
        all_second(f, b).wait_recv()
        modes[f] = z_transform(r2.at[f, b], h, g_high, g_low)

    def mixing(b):
        weights = [[mix[a, c] for c in range(F)] for a in range(F)]

        def plane(kx, carry):
            shift = sx[32 * left + 8 * b + kx]
            for part in range(4):
                rows = pl.ds(8 * part, 8)
                weight = 1.0 / (base[rows, :] + shift)
                other = 1.0 - weight
                old = [modes[a, kx, rows, :] for a in range(F)]
                for a in range(F):
                    mixed = weights[a][0] * old[0]
                    for c in range(1, F):
                        mixed += weights[a][c] * old[c]
                    out[a, 8 * b + kx, rows, :] = weight * old[a] + other * mixed
            return carry

        lax.fori_loop(0, 8, plane, 0)

    def prepare_last():
        weights = [[mix[a, c] for c in range(F)] for a in range(F)]

        def plane(kx, carry):
            shift = sx[32 * left + 8 * (BLOCKS - 1) + kx]
            for part in range(4):
                rows = pl.ds(8 * part, 8)
                weight = 1.0 / (base[rows, :] + shift)
                other = 1.0 - weight
                old = [modes[a, kx, rows, :] for a in range(F - 1)]
                for a in range(F):
                    mixed = weights[a][0] * old[0]
                    for c in range(1, F - 1):
                        mixed += weights[a][c] * old[c]
                    first_terms = other * mixed
                    last_term = weights[a][F - 1] * other
                    if a < F - 1:
                        partial[a, kx, rows, :] = weight * old[a] + first_terms
                        slope[a, kx, rows, :] = last_term
                    else:
                        partial[a, kx, rows, :] = first_terms
                        slope[a, kx, rows, :] = last_term + weight
            return carry

        lax.fori_loop(0, 8, plane, 0)

    lax.fori_loop(0, F, opening, 0)

    def send_chunk(c, carry):
        send_first(c % F, c // F)
        return carry

    lax.fori_loop(F, AHEAD, send_chunk, 0)
    small[1].wait()

    def step(i, carry):
        @pl.when(i < F * BLOCKS)
        def _():
            along_y(i % F, i // F)

        @pl.when(i >= LAG)
        def _():
            j = i - LAG
            all_first(j % F, j // F).wait_send()
            all_second(j % F, j // F).wait_send()
            along_z(j % F, j // F)

            @pl.when(j % F == F - 1)
            def _():
                mixing(j // F)

        @pl.when(i < F)
        def _():
            along_x(i, 1)

        @pl.when(i + AHEAD < F * BLOCKS)
        def _():
            send_chunk(i + AHEAD, 0)

        @pl.when(i == F)
        def _():
            for copy in small[2:]:
                copy.wait()
            for ky in range(32):
                base[pl.ds(ky, 1), :] = 1.0 + (sz[...] + sy[32 * right + ky])

        return carry

    lax.fori_loop(0, LAST + LAG, step, 0)
    prepare_last()
    all_first(F - 1, BLOCKS - 1).wait_send()
    all_second(F - 1, BLOCKS - 1).wait_send()
    all_second(F - 1, BLOCKS - 1).wait_recv()
    tail[...] = r2[F - 1, BLOCKS - 1]


def write_kernel(modes, h, partial, slope, tail, out, last, g_high, g_low, sems):
    done = BLOCKS - 1
    copies = [
        pltpu.make_async_copy(modes.at[f, pl.ds(8 * b, 8)], out.at[f, pl.ds(8 * b, 8)], sems.at[f, b])
        for f in range(F)
        for b in range(done)
    ]
    for copy in copies:
        copy.start()
    last[F - 1] = z_transform(tail, h, g_high, g_low)
    for kx in range(8):
        for part in range(4):
            rows = pl.ds(8 * part, 8)
            old = last[F - 1, kx, rows, :]
            for a in range(F):
                last[a, kx, rows, :] = partial[a, kx, rows, :] + slope[a, kx, rows, :] * old
    for f in range(F):
        copies.append(pltpu.make_async_copy(last.at[f], out.at[f, pl.ds(8 * done, 8)], sems.at[f, done]))
        copies[-1].start()
    for copy in copies:
        copy.wait()


def body(species, coupling, symbol_x, symbol_y, symbol_z):
    hbm = pl.BlockSpec(memory_space=pltpu.HBM)
    vmem = pl.BlockSpec(memory_space=pltpu.VMEM)
    wide = basis_table(512)
    rows = np.arange(512).reshape(16, BLOCKS, 8).transpose(1, 0, 2).reshape(-1)
    tables_x = np.stack(halves(wide[rows]))
    tables = np.stack(halves(basis_table(256)))
    flat = jnp.transpose(species, (0, 2, 3, 1)).reshape(F * 512, 512)
    arrays = (flat, tables_x, tables, coupling, symbol_x, symbol_y, symbol_z.reshape(1, 256))
    results = pl.pallas_call(
        kernel,
        out_shape=(
            pltpu.VMEM((F, 8 * (BLOCKS - 1), 32, 256), jnp.float32),
            pltpu.VMEM((2, 256, 256), jnp.bfloat16),
            pltpu.VMEM((F, 8, 32, 256), jnp.float32),
            pltpu.VMEM((F, 8, 32, 256), jnp.float32),
            pltpu.VMEM((8, 32, 256), jnp.float32),
        ),
        in_specs=[hbm] * 7,
        out_specs=[vmem] * 5,
        scratch_shapes=[
            pltpu.VMEM((F * 4 * 512, 128), jnp.float32),
            pltpu.VMEM((2, 512, 512), jnp.bfloat16),
            pltpu.VMEM((F, 512, 512), jnp.bfloat16),
            pltpu.VMEM((F, 512, 512), jnp.bfloat16),
            pltpu.VMEM((F, BLOCKS, 16, 8, 512), jnp.float32),
            pltpu.VMEM((F, BLOCKS, 16, 8, 512), jnp.float32),
            pltpu.VMEM((512, 128), jnp.float32),
            pltpu.VMEM((256, 256), jnp.bfloat16),
            pltpu.VMEM((256, 256), jnp.bfloat16),
            pltpu.VMEM((F, BLOCKS, 8, 32, 256), jnp.float32),
            pltpu.VMEM((F, BLOCKS, 8, 32, 256), jnp.float32),
            pltpu.VMEM((256, 256), jnp.bfloat16),
            pltpu.VMEM((256, 256), jnp.bfloat16),
            pltpu.VMEM((F, 8, 32, 256), jnp.float32),
            pltpu.VMEM((32, 256), jnp.float32),
            pltpu.SMEM((F, F), jnp.float32),
            pltpu.SMEM((512,), jnp.float32),
            pltpu.SMEM((256,), jnp.float32),
            pltpu.VMEM((1, 256), jnp.float32),
            pltpu.SemaphoreType.DMA((F, 4)),
            pltpu.SemaphoreType.DMA((6,)),
            pltpu.SemaphoreType.DMA((F, BLOCKS)),
            pltpu.SemaphoreType.DMA((F, BLOCKS)),
            pltpu.SemaphoreType.DMA((F, BLOCKS)),
            pltpu.SemaphoreType.DMA((F, BLOCKS)),
        ],
        compiler_params=pltpu.CompilerParams(
            collective_id=0, has_side_effects=True, vmem_limit_bytes=40 * 2**20
        ),
        name="transform",
    )(*(pltpu.with_memory_space_constraint(a, pltpu.HBM) for a in arrays))
    return pl.pallas_call(
        write_kernel,
        out_shape=jax.ShapeDtypeStruct((F, 32, 32, 256), jnp.float32),
        in_specs=[vmem] * 5,
        out_specs=hbm,
        scratch_shapes=[
            pltpu.VMEM((F, 8, 32, 256), jnp.float32),
            pltpu.VMEM((256, 256), jnp.bfloat16),
            pltpu.VMEM((256, 256), jnp.bfloat16),
            pltpu.SemaphoreType.DMA((F, BLOCKS)),
        ],
        compiler_params=pltpu.CompilerParams(vmem_limit_bytes=4 * 2**20),
        name="write",
    )(*results)


def solution(mesh):
    in_specs = (P(None, None, "left", "right"), P(), P(), P(), P())
    out_specs = P(None, "left", "right", None)
    return jax.shard_map(body, mesh=mesh, in_specs=in_specs, out_specs=out_specs, check_vma=False)
```

```python
import jax
import jax.numpy as jnp
import numpy as np
from jax import lax
from jax.experimental import pallas as pl
from jax.experimental.pallas import tpu as pltpu
from jax.sharding import PartitionSpec as P

MESH = pl.DeviceIdType.MESH
F = 4
BLOCKS = 4
LAG = 5
AHEAD = 8
CHUNKS = 2 * F * BLOCKS
LAST = F * BLOCKS - 1

LEFT_STEPS = [(dz, dx) for dx in (2, 1, 3, 0) for dz in (2, 1, 3, 0) if (dz, dx) != (0, 0)]
RIGHT_STEPS = [(dy, dc) for dy in (2, 1, 3, 0) for dc in (0, 1) if (dy, dc) != (0, 0)]


def basis_table(count):
    rank = np.arange(count)
    angle = 2.0 * np.pi / count * (rank[:, None] * rank[None, :] % count)
    return ((np.cos(angle) + np.sin(angle)) * count**-0.5).astype(np.float32)


def halves(table):
    high = table.astype(jnp.bfloat16)
    low = (table - high.astype(np.float32)).astype(jnp.bfloat16)
    return high, low


def split(values):
    high = values.astype(jnp.bfloat16)
    return high, (values - high.astype(jnp.float32)).astype(jnp.bfloat16)


def dot_nt(a, b):
    return lax.dot_general(a, b, (((1,), (1,)), ((), ())), preferred_element_type=jnp.float32)


def dot_nn(a, b):
    return lax.dot_general(a, b, (((1,), (0,)), ((), ())), preferred_element_type=jnp.float32)


def gather_blocks(arrays, width):
    count = len(arrays)
    position = lax.broadcasted_iota(jnp.int32, arrays[0].shape, 1) // width
    moved = [arrays[-w % count] for w in range(count)]
    bit = 1
    while bit < count:
        odd = position // bit % 2 == 1
        moved = [jnp.where(odd, moved[(w - bit) % count], moved[w]) for w in range(count)]
        bit *= 2
    return [moved[0]] + [pltpu.roll(moved[w], 128 - width * w, 1) for w in range(1, count)]


def z_transform(pieces, h, g_high, g_low):
    for half in range(2):
        arrays = [pieces[half, i] for i in range(8)]
        for i, array in enumerate(gather_blocks(arrays, 16)):
            high, low = split(array)
            g_high[pl.ds(32 * i, 32), pl.ds(128 * half, 128)] = high
            g_low[pl.ds(32 * i, 32), pl.ds(128 * half, 128)] = low
    part = dot_nn(g_high[...], h[0])
    part += dot_nn(g_low[...], h[0])
    part += dot_nn(g_high[...], h[1])
    return part.reshape(8, 32, 256)


def kernel(
    species, tables_x, tables, tables_z, coupling, symbol_x, symbol_y, symbol_z, out, hz, partial, slope, tail,
    grid, hx, h, d_high, d_low, s1, r1, d2, e_high, e_low, s2, r2, g_high, g_low, modes, base, mix, sx, sy, sz,
    in_sem, h_sem, send1, recv1, send2, recv2,
):
    left, right = lax.axis_index("left"), lax.axis_index("right")
    z, x = left // 4, left % 4
    y, core = right // 2, right % 2
    left_peers = [lax.rem(z + dz, 4) * 4 + lax.rem(x + dx, 4) for dz, dx in LEFT_STEPS]
    right_peers = [lax.rem(y + dy, 4) * 2 + lax.rem(core + dc, 2) for dy, dc in RIGHT_STEPS]

    def load(f, t):
        return pltpu.make_async_copy(
            species.at[pl.ds(512 * f, 512), pl.ds(128 * t, 128)],
            grid.at[pl.ds((4 * f + t) * 512, 512)],
            in_sem.at[f],
        )

    def loaded(f):
        rows = pl.ds(2048 * f, 2048)
        pltpu.make_async_copy(grid.at[rows], grid.at[rows], in_sem.at[f]).wait()

    small = [
        pltpu.make_async_copy(a, b, h_sem.at[i])
        for i, (a, b) in enumerate(
            [(tables_x, hx), (tables, h), (tables_z, hz), (coupling, mix), (symbol_x, sx), (symbol_y, sy), (symbol_z, sz)]
        )
    ]
    for t in range(4):
        load(0, t).start()
    small[0].start()
    for f in range(1, F):
        for t in range(4):
            load(f, t).start()
    for copy in small[1:]:
        copy.start()

    barrier = pltpu.get_barrier_semaphore()
    for peer in left_peers:
        pl.semaphore_signal(barrier, inc=1, device_id=(peer, right), device_id_type=MESH)
    for peer in right_peers:
        pl.semaphore_signal(barrier, inc=1, device_id=(left, peer), device_id_type=MESH)

    def first(f, b, half, k):
        return pltpu.make_async_remote_copy(
            src_ref=s1.at[f, b, half, left_peers[k]],
            dst_ref=r1.at[f, b, half, left],
            send_sem=send1.at[b],
            recv_sem=recv1.at[f, b, half],
            device_id=(left_peers[k], right),
            device_id_type=MESH,
        )

    def second(f, b, half, k):
        return pltpu.make_async_remote_copy(
            src_ref=s2.at[f, b, half, right_peers[k]],
            dst_ref=r2.at[f, b, half, right],
            send_sem=send2.at[b],
            recv_sem=recv2.at[f, b],
            device_id=(left, right_peers[k]),
            device_id_type=MESH,
        )

    def all_first(f, b, half):
        return pltpu.make_async_remote_copy(
            src_ref=s1.at[f, b, half, pl.ds(0, 15)],
            dst_ref=r1.at[f, b, half, pl.ds(0, 15)],
            send_sem=send1.at[b],
            recv_sem=recv1.at[f, b, half],
            device_id=(left_peers[0], right),
            device_id_type=MESH,
        )

    def all_second(f, b):
        return pltpu.make_async_remote_copy(
            src_ref=s2.at[f, b, :, pl.ds(0, 7)],
            dst_ref=r2.at[f, b, :, pl.ds(0, 7)],
            send_sem=send2.at[b],
            recv_sem=recv2.at[f, b],
            device_id=(left, right_peers[0]),
            device_id_type=MESH,
        )

    def send_first(c):
        for k in range(len(left_peers)):
            first(c // 2 % F, c // (2 * F), c % 2, k).start()

    def sent(b):
        pltpu.make_async_remote_copy(
            src_ref=s1.at[:, b, :, pl.ds(0, 15)],
            dst_ref=r1.at[:, b, :, pl.ds(0, 15)],
            send_sem=send1.at[b],
            recv_sem=recv1.at[0, b, 0],
            device_id=(left_peers[0], right),
            device_id_type=MESH,
        ).wait_send()
        pltpu.make_async_remote_copy(
            src_ref=s2.at[:, b, :, pl.ds(0, 7)],
            dst_ref=r2.at[:, b, :, pl.ds(0, 7)],
            send_sem=send2.at[b],
            recv_sem=recv2.at[0, b],
            device_id=(left, right_peers[0]),
            device_id_type=MESH,
        ).wait_send()

    def arrange(f):
        loaded(f)
        for t in range(4):
            for zi in range(32):
                rows = grid[pl.ds((4 * f + t) * 512 + zi, 16, stride=32), :]
                high, low = split(rows)
                place = pl.multiple_of(16 * (zi // 8 * 8 + lax.rem(zi % 8 + left, 8)), 16)
                d_high[f, pl.ds(place, 16), pl.ds(128 * t, 128)] = high
                d_low[f, pl.ds(place, 16), pl.ds(128 * t, 128)] = low

    def along_x(f, p):
        rows = pl.ds(pl.multiple_of(256 * p, 256), 256)
        part = dot_nt(hx[0, rows, :], d_high[f])
        part += dot_nt(hx[0, rows, :], d_low[f])
        part += dot_nt(hx[1, rows, :], d_high[f])
        for half in range(2):
            s1[f, pl.ds(2 * p, 2), half] = part[:, 256 * half : 256 * half + 256].reshape(2, 16, 8, 256)
            for i in range(2):
                r1[f, 2 * p + i, half, left] = s1[f, 2 * p + i, half, left]

    def opening(f, carry):
        arrange(f)

        @pl.when(f == 0)
        def _():
            small[0].wait()

        along_x(f, 0)

        @pl.when(f == 0)
        def _():
            pl.semaphore_wait(barrier, len(left_peers) + len(right_peers))

        send_first(2 * f)
        send_first(2 * f + 1)
        return carry

    def along_y(f, b, half):
        all_first(f, b, half).wait_recv()
        for t in range(2):
            for g in range(2):
                arrays = [r1[f, b, half, 8 * g + i, :, pl.ds(128 * t, 128)] for i in range(8)]
                for i, array in enumerate(gather_blocks(arrays, 16)):
                    d2[pl.ds(128 * g + 8 * (8 * t + i), 8), :] = array
        for g in range(2):
            for kx in range(8):
                high, low = split(d2[pl.ds(128 * g + kx, 16, stride=8), :])
                place = pl.multiple_of(16 * lax.rem(kx + right, 8), 16)
                e_high[pl.ds(place, 16), pl.ds(128 * g, 128)] = high
                e_low[pl.ds(place, 16), pl.ds(128 * g, 128)] = low
        both = dot_nt(h[...].reshape(512, 256), e_high[...])
        part = both[:256] + both[256:] + dot_nt(h[0], e_low[...])
        s2[f, b, half] = part.reshape(8, 32, 128)
        r2[f, b, half, right] = s2[f, b, half, right]
        for k in range(len(right_peers)):
            second(f, b, half, k).start()

    def along_z(f, b):
        all_second(f, b).wait_recv()
        modes[b % 2, f] = z_transform(r2.at[f, b], hz, g_high, g_low)

    def mixing(b, kx):
        weights = [[mix[a, c] for c in range(F)] for a in range(F)]
        shift = sx[32 * left + 8 * b + kx]
        for part in range(4):
            rows = pl.ds(8 * part, 8)
            weight = 1.0 / (base[rows, :] + shift)
            other = 1.0 - weight
            old = [modes[b % 2, a, kx, rows, :] for a in range(F)]
            for a in range(F):
                mixed = weights[a][0] * old[0]
                for c in range(1, F):
                    mixed += weights[a][c] * old[c]
                out[a, 8 * b + kx, rows, :] = weight * old[a] + other * mixed

    def prepare_last():
        weights = [[mix[a, c] for c in range(F)] for a in range(F)]

        def plane(kx, carry):
            shift = sx[32 * left + 8 * (BLOCKS - 1) + kx]
            for part in range(4):
                rows = pl.ds(8 * part, 8)
                weight = 1.0 / (base[rows, :] + shift)
                other = 1.0 - weight
                old = [modes[(BLOCKS - 1) % 2, a, kx, rows, :] for a in range(F - 1)]
                for a in range(F):
                    mixed = weights[a][0] * old[0]
                    for c in range(1, F - 1):
                        mixed += weights[a][c] * old[c]
                    first_terms = other * mixed
                    last_term = weights[a][F - 1] * other
                    if a < F - 1:
                        partial[a, kx, rows, :] = weight * old[a] + first_terms
                        slope[a, kx, rows, :] = last_term
                    else:
                        partial[a, kx, rows, :] = first_terms
                        slope[a, kx, rows, :] = last_term + weight
            return carry

        lax.fori_loop(0, 8, plane, 0)

    lax.fori_loop(0, F, opening, 0)

    def send_chunk(c, carry):
        send_first(c)
        return carry

    lax.fori_loop(2 * F, AHEAD, send_chunk, 0)
    small[1].wait()

    def step(i, carry):
        @pl.when(i < CHUNKS)
        def _():
            along_y(i // 2 % F, i // (2 * F), i % 2)

        @pl.when(i < F)
        def _():
            along_x(i, 1)

        @pl.when(i + AHEAD < CHUNKS)
        def _():
            send_first(i + AHEAD)

        @pl.when(i == F)
        def _():
            for copy in small[2:]:
                copy.wait()
            for ky in range(32):
                base[pl.ds(ky, 1), :] = 1.0 + (sz[...] + sy[32 * right + ky])

        @pl.when(((i + LAG) % 2 == 1) & (i > LAG) & (i < 2 * LAST + LAG))
        def _():
            j = (i - LAG - 1) // 2
            along_z(j % F, j // F)

        plane = i - 2 * F - LAG

        @pl.when(plane >= 0)
        def _():
            mixing(plane // 8, plane % 8)

        return carry

    lax.fori_loop(0, CHUNKS + LAG, step, 0)
    prepare_last()
    for b in range(BLOCKS):
        sent(b)
    all_second(F - 1, BLOCKS - 1).wait_recv()
    tail[...] = r2[F - 1, BLOCKS - 1]


def write_kernel(modes, h, partial, slope, tail, out, last, g_high, g_low, sems):
    done = 8 * (BLOCKS - 1)
    copies = [
        pltpu.make_async_copy(modes.at[f], out.at[f, pl.ds(0, done)], sems.at[0, f]) for f in range(F)
    ]
    for copy in copies:
        copy.start()
    last[F - 1] = z_transform(tail, h, g_high, g_low)
    for kx in range(8):
        for part in range(4):
            rows = pl.ds(8 * part, 8)
            old = last[F - 1, kx, rows, :]
            for a in range(F):
                last[a, kx, rows, :] = partial[a, kx, rows, :] + slope[a, kx, rows, :] * old
    for f in range(F):
        copies.append(pltpu.make_async_copy(last.at[f], out.at[f, pl.ds(done, 8)], sems.at[1, f]))
        copies[-1].start()
    for copy in copies:
        copy.wait()


def body(species, coupling, symbol_x, symbol_y, symbol_z):
    hbm = pl.BlockSpec(memory_space=pltpu.HBM)
    vmem = pl.BlockSpec(memory_space=pltpu.VMEM)
    wide = basis_table(512)
    rows = np.arange(512).reshape(16, BLOCKS, 8).transpose(1, 0, 2).reshape(-1)
    tables_x = np.stack(halves(wide[rows]))
    tables = np.stack(halves(basis_table(256)))
    rows = np.arange(256).reshape(8, 2, 16).transpose(1, 0, 2).reshape(-1)
    tables_z = tables[:, rows]
    flat = jnp.transpose(species, (0, 2, 3, 1)).reshape(F * 512, 512)
    arrays = (flat, tables_x, tables, tables_z, coupling, symbol_x, symbol_y, symbol_z.reshape(1, 256))
    results = pl.pallas_call(
        kernel,
        out_shape=(
            pltpu.VMEM((F, 8 * (BLOCKS - 1), 32, 256), jnp.float32),
            pltpu.VMEM((2, 256, 256), jnp.bfloat16),
            pltpu.VMEM((F, 8, 32, 256), jnp.float32),
            pltpu.VMEM((F, 8, 32, 256), jnp.float32),
            pltpu.VMEM((2, 8, 32, 128), jnp.float32),
        ),
        in_specs=[hbm] * 8,
        out_specs=[vmem] * 5,
        scratch_shapes=[
            pltpu.VMEM((F * 4 * 512, 128), jnp.float32),
            pltpu.VMEM((2, 512, 512), jnp.bfloat16),
            pltpu.VMEM((2, 256, 256), jnp.bfloat16),
            pltpu.VMEM((F, 512, 512), jnp.bfloat16),
            pltpu.VMEM((F, 512, 512), jnp.bfloat16),
            pltpu.VMEM((F, BLOCKS, 2, 16, 8, 256), jnp.float32),
            pltpu.VMEM((F, BLOCKS, 2, 16, 8, 256), jnp.float32),
            pltpu.VMEM((256, 128), jnp.float32),
            pltpu.VMEM((128, 256), jnp.bfloat16),
            pltpu.VMEM((128, 256), jnp.bfloat16),
            pltpu.VMEM((F, BLOCKS, 2, 8, 32, 128), jnp.float32),
            pltpu.VMEM((F, BLOCKS, 2, 8, 32, 128), jnp.float32),
            pltpu.VMEM((256, 256), jnp.bfloat16),
            pltpu.VMEM((256, 256), jnp.bfloat16),
            pltpu.VMEM((2, F, 8, 32, 256), jnp.float32),
            pltpu.VMEM((32, 256), jnp.float32),
            pltpu.SMEM((F, F), jnp.float32),
            pltpu.SMEM((512,), jnp.float32),
            pltpu.SMEM((256,), jnp.float32),
            pltpu.VMEM((1, 256), jnp.float32),
            pltpu.SemaphoreType.DMA((F,)),
            pltpu.SemaphoreType.DMA((7,)),
            pltpu.SemaphoreType.DMA((BLOCKS,)),
            pltpu.SemaphoreType.DMA((F, BLOCKS, 2)),
            pltpu.SemaphoreType.DMA((BLOCKS,)),
            pltpu.SemaphoreType.DMA((F, BLOCKS)),
        ],
        compiler_params=pltpu.CompilerParams(
            collective_id=0, has_side_effects=True, vmem_limit_bytes=40 * 2**20
        ),
        name="transform",
    )(*(pltpu.with_memory_space_constraint(a, pltpu.HBM) for a in arrays))
    return pl.pallas_call(
        write_kernel,
        out_shape=jax.ShapeDtypeStruct((F, 32, 32, 256), jnp.float32),
        in_specs=[vmem] * 5,
        out_specs=hbm,
        scratch_shapes=[
            pltpu.VMEM((F, 8, 32, 256), jnp.float32),
            pltpu.VMEM((256, 256), jnp.bfloat16),
            pltpu.VMEM((256, 256), jnp.bfloat16),
            pltpu.SemaphoreType.DMA((2, F)),
        ],
        compiler_params=pltpu.CompilerParams(vmem_limit_bytes=4 * 2**20),
        name="write",
    )(*results)


def solution(mesh):
    in_specs = (P(None, None, "left", "right"), P(), P(), P(), P())
    out_specs = P(None, "left", "right", None)
    return jax.shard_map(body, mesh=mesh, in_specs=in_specs, out_specs=out_specs, check_vma=False)
```

```python
import jax
import jax.numpy as jnp
import numpy as np
from jax import lax
from jax.experimental import pallas as pl
from jax.experimental.pallas import tpu as pltpu
from jax.sharding import PartitionSpec as P

MESH = pl.DeviceIdType.MESH
F = 4
BLOCKS = 4
LAG = 5
AHEAD = 8
CHUNKS = 2 * F * BLOCKS
LAST = F * BLOCKS - 1

LEFT_STEPS = [(dz, dx) for dx in (2, 1, 3, 0) for dz in (2, 1, 3, 0) if (dz, dx) != (0, 0)]
RIGHT_STEPS = [(dy, dc) for dc in (0, 1) for dy in (2, 1, 3, 0) if (dy, dc) != (0, 0)]


def basis_table(count):
    rank = np.arange(count)
    angle = 2.0 * np.pi / count * (rank[:, None] * rank[None, :] % count)
    return ((np.cos(angle) + np.sin(angle)) * count**-0.5).astype(np.float32)


def halves(table):
    high = table.astype(jnp.bfloat16)
    low = (table - high.astype(np.float32)).astype(jnp.bfloat16)
    return high, low


def split(values):
    high = values.astype(jnp.bfloat16)
    return high, (values - high.astype(jnp.float32)).astype(jnp.bfloat16)


def dot_nt(a, b):
    return lax.dot_general(a, b, (((1,), (1,)), ((), ())), preferred_element_type=jnp.float32)


def dot_nn(a, b):
    return lax.dot_general(a, b, (((1,), (0,)), ((), ())), preferred_element_type=jnp.float32)


def gather_blocks(arrays, width):
    count = len(arrays)
    position = lax.broadcasted_iota(jnp.int32, arrays[0].shape, 1) // width
    moved = [arrays[-w % count] for w in range(count)]
    bit = 1
    while bit < count:
        odd = position // bit % 2 == 1
        moved = [jnp.where(odd, moved[(w - bit) % count], moved[w]) for w in range(count)]
        bit *= 2
    return [moved[0]] + [pltpu.roll(moved[w], 128 - width * w, 1) for w in range(1, count)]


def z_transform(pieces, h, g_high, g_low):
    for half in range(2):
        arrays = [pieces[half, i] for i in range(8)]
        for i, array in enumerate(gather_blocks(arrays, 16)):
            high, low = split(array)
            g_high[pl.ds(32 * i, 32), pl.ds(128 * half, 128)] = high
            g_low[pl.ds(32 * i, 32), pl.ds(128 * half, 128)] = low
    part = dot_nn(g_high[...], h[0])
    part += dot_nn(g_low[...], h[0])
    part += dot_nn(g_high[...], h[1])
    return part.reshape(8, 32, 256)


def kernel(
    species, tables_x, tables, tables_z, coupling, symbol_x, symbol_y, symbol_z, out, hz, partial, slope, tail,
    grid, hx, h, d_high, d_low, s1, r1, d2, e_high, e_low, s2, r2, g_high, g_low, modes, base, mix, sx, sy, sz,
    in_sem, h_sem, send1, recv1, send2, recv2,
):
    left, right = lax.axis_index("left"), lax.axis_index("right")
    z, x = left // 4, left % 4
    y, core = right // 2, right % 2
    left_peers = [lax.rem(z + dz, 4) * 4 + lax.rem(x + dx, 4) for dz, dx in LEFT_STEPS]
    right_peers = [lax.rem(y + dy, 4) * 2 + lax.rem(core + dc, 2) for dy, dc in RIGHT_STEPS]

    barrier = pltpu.get_barrier_semaphore()
    for peer in left_peers:
        pl.semaphore_signal(barrier, inc=1, device_id=(peer, right), device_id_type=MESH)
    for peer in right_peers:
        pl.semaphore_signal(barrier, inc=1, device_id=(left, peer), device_id_type=MESH)

    def load(f, t):
        return pltpu.make_async_copy(
            species.at[pl.ds(512 * f, 512), pl.ds(128 * t, 128)],
            grid.at[pl.ds((4 * f + t) * 512, 512)],
            in_sem.at[f],
        )

    def loaded(f):
        rows = pl.ds(2048 * f, 2048)
        pltpu.make_async_copy(grid.at[rows], grid.at[rows], in_sem.at[f]).wait()

    small = [
        pltpu.make_async_copy(a, b, h_sem.at[i])
        for i, (a, b) in enumerate(
            [(tables_x, hx), (tables, h), (tables_z, hz), (coupling, mix), (symbol_x, sx), (symbol_y, sy), (symbol_z, sz)]
        )
    ]
    for t in range(4):
        load(0, t).start()
    small[0].start()
    for f in range(1, F):
        for t in range(4):
            load(f, t).start()
    for copy in small[1:]:
        copy.start()

    def first(f, b, half, k):
        return pltpu.make_async_remote_copy(
            src_ref=s1.at[f, b, half, left_peers[k]],
            dst_ref=r1.at[f, b, half, left],
            send_sem=send1.at[b],
            recv_sem=recv1.at[f, b, half],
            device_id=(left_peers[k], right),
            device_id_type=MESH,
        )

    def second(f, b, half, k):
        return pltpu.make_async_remote_copy(
            src_ref=s2.at[f, b, half, right_peers[k]],
            dst_ref=r2.at[f, b, half, right],
            send_sem=send2.at[b],
            recv_sem=recv2.at[f, b],
            device_id=(left, right_peers[k]),
            device_id_type=MESH,
        )

    def all_first(f, b, half):
        return pltpu.make_async_remote_copy(
            src_ref=s1.at[f, b, half, pl.ds(0, 15)],
            dst_ref=r1.at[f, b, half, pl.ds(0, 15)],
            send_sem=send1.at[b],
            recv_sem=recv1.at[f, b, half],
            device_id=(left_peers[0], right),
            device_id_type=MESH,
        )

    def all_second(f, b):
        return pltpu.make_async_remote_copy(
            src_ref=s2.at[f, b, :, pl.ds(0, 7)],
            dst_ref=r2.at[f, b, :, pl.ds(0, 7)],
            send_sem=send2.at[b],
            recv_sem=recv2.at[f, b],
            device_id=(left, right_peers[0]),
            device_id_type=MESH,
        )

    def send_first(c):
        for k in range(len(left_peers)):
            first(c // 2 % F, c // (2 * F), c % 2, k).start()

    def sent(b):
        pltpu.make_async_remote_copy(
            src_ref=s1.at[:, b, :, pl.ds(0, 15)],
            dst_ref=r1.at[:, b, :, pl.ds(0, 15)],
            send_sem=send1.at[b],
            recv_sem=recv1.at[0, b, 0],
            device_id=(left_peers[0], right),
            device_id_type=MESH,
        ).wait_send()
        pltpu.make_async_remote_copy(
            src_ref=s2.at[:, b, :, pl.ds(0, 7)],
            dst_ref=r2.at[:, b, :, pl.ds(0, 7)],
            send_sem=send2.at[b],
            recv_sem=recv2.at[0, b],
            device_id=(left, right_peers[0]),
            device_id_type=MESH,
        ).wait_send()

    def arrange(f):
        loaded(f)
        for t in range(4):
            for zi in range(32):
                rows = grid[pl.ds((4 * f + t) * 512 + zi, 16, stride=32), :]
                high, low = split(rows)
                place = pl.multiple_of(16 * (zi // 8 * 8 + lax.rem(zi % 8 + left, 8)), 16)
                d_high[f, pl.ds(place, 16), pl.ds(128 * t, 128)] = high
                d_low[f, pl.ds(place, 16), pl.ds(128 * t, 128)] = low

    def along_x(f, p):
        rows = pl.ds(pl.multiple_of(256 * p, 256), 256)
        part = dot_nt(hx[0, rows, :], d_high[f])
        part += dot_nt(hx[0, rows, :], d_low[f])
        part += dot_nt(hx[1, rows, :], d_high[f])
        for half in range(2):
            s1[f, pl.ds(2 * p, 2), half] = part[:, 256 * half : 256 * half + 256].reshape(2, 16, 8, 256)
            for i in range(2):
                r1[f, 2 * p + i, half, left] = s1[f, 2 * p + i, half, left]

    def opening(f, carry):
        arrange(f)

        @pl.when(f == 0)
        def _():
            small[0].wait()

        along_x(f, 0)

        @pl.when(f == 0)
        def _():
            pl.semaphore_wait(barrier, len(left_peers) + len(right_peers))

        send_first(2 * f)
        send_first(2 * f + 1)
        return carry

    def along_y(f, b, half):
        all_first(f, b, half).wait_recv()
        for t in range(2):
            for g in range(2):
                arrays = [r1[f, b, half, 8 * g + i, :, pl.ds(128 * t, 128)] for i in range(8)]
                for i, array in enumerate(gather_blocks(arrays, 16)):
                    d2[pl.ds(128 * g + 8 * (8 * t + i), 8), :] = array
        for g in range(2):
            for kx in range(8):
                high, low = split(d2[pl.ds(128 * g + kx, 16, stride=8), :])
                place = pl.multiple_of(16 * lax.rem(kx + right, 8), 16)
                e_high[pl.ds(place, 16), pl.ds(128 * g, 128)] = high
                e_low[pl.ds(place, 16), pl.ds(128 * g, 128)] = low
        both = dot_nt(h[...].reshape(512, 256), e_high[...])
        part = both[:256] + both[256:] + dot_nt(h[0], e_low[...])
        s2[f, b, half] = part.reshape(8, 32, 128)
        for k in range(len(right_peers)):
            second(f, b, half, k).start()
        r2[f, b, half, right] = s2[f, b, half, right]

    def along_z(f, b):
        all_second(f, b).wait_recv()
        modes[b % 2, f] = z_transform(r2.at[f, b], hz, g_high, g_low)

    def mixing(b, kx):
        weights = [[mix[a, c] for c in range(F)] for a in range(F)]
        shift = sx[32 * left + 8 * b + kx]
        for part in range(4):
            rows = pl.ds(8 * part, 8)
            weight = 1.0 / (base[rows, :] + shift)
            other = 1.0 - weight
            old = [modes[b % 2, a, kx, rows, :] for a in range(F)]
            for a in range(F):
                mixed = weights[a][0] * old[0]
                for c in range(1, F):
                    mixed += weights[a][c] * old[c]
                out[a, 8 * b + kx, rows, :] = weight * old[a] + other * mixed

    def prepare_last():
        weights = [[mix[a, c] for c in range(F)] for a in range(F)]

        def plane(kx, carry):
            shift = sx[32 * left + 8 * (BLOCKS - 1) + kx]
            for part in range(4):
                rows = pl.ds(8 * part, 8)
                weight = 1.0 / (base[rows, :] + shift)
                other = 1.0 - weight
                old = [modes[(BLOCKS - 1) % 2, a, kx, rows, :] for a in range(F - 1)]
                for a in range(F):
                    mixed = weights[a][0] * old[0]
                    for c in range(1, F - 1):
                        mixed += weights[a][c] * old[c]
                    first_terms = other * mixed
                    last_term = weights[a][F - 1] * other
                    if a < F - 1:
                        partial[a, kx, rows, :] = weight * old[a] + first_terms
                        slope[a, kx, rows, :] = last_term
                    else:
                        partial[a, kx, rows, :] = first_terms
                        slope[a, kx, rows, :] = last_term + weight
            return carry

        lax.fori_loop(0, 8, plane, 0)

    lax.fori_loop(0, F, opening, 0)

    def send_chunk(c, carry):
        send_first(c)
        return carry

    lax.fori_loop(2 * F, AHEAD, send_chunk, 0)
    small[1].wait()

    def step(i, carry):
        @pl.when(i < CHUNKS)
        def _():
            along_y(i // 2 % F, i // (2 * F), i % 2)

        @pl.when(i < F)
        def _():
            along_x(i, 1)

        @pl.when(i + AHEAD < CHUNKS)
        def _():
            send_first(i + AHEAD)

        @pl.when(i == F)
        def _():
            for copy in small[2:]:
                copy.wait()
            for ky in range(32):
                base[pl.ds(ky, 1), :] = 1.0 + (sz[...] + sy[32 * right + ky])

        @pl.when(((i + LAG) % 2 == 1) & (i > LAG) & (i < 2 * LAST + LAG))
        def _():
            j = (i - LAG - 1) // 2
            along_z(j % F, j // F)

        plane = i - 2 * F - LAG

        @pl.when(plane >= 0)
        def _():
            mixing(plane // 8, plane % 8)

        return carry

    lax.fori_loop(0, CHUNKS + LAG, step, 0)
    prepare_last()
    for b in range(BLOCKS):
        sent(b)
    all_second(F - 1, BLOCKS - 1).wait_recv()
    tail[...] = r2[F - 1, BLOCKS - 1]


def write_kernel(modes, h, partial, slope, tail, out, last, g_high, g_low, sems):
    done = 8 * (BLOCKS - 1)
    copies = [
        pltpu.make_async_copy(modes.at[f], out.at[f, pl.ds(0, done)], sems.at[0, f]) for f in range(F)
    ]
    for copy in copies:
        copy.start()
    last[F - 1] = z_transform(tail, h, g_high, g_low)
    for kx in range(8):
        for part in range(4):
            rows = pl.ds(8 * part, 8)
            old = last[F - 1, kx, rows, :]
            for a in range(F):
                last[a, kx, rows, :] = partial[a, kx, rows, :] + slope[a, kx, rows, :] * old
    for f in range(F):
        copies.append(pltpu.make_async_copy(last.at[f], out.at[f, pl.ds(done, 8)], sems.at[1, f]))
        copies[-1].start()
    for copy in copies:
        copy.wait()


def body(species, coupling, symbol_x, symbol_y, symbol_z):
    hbm = pl.BlockSpec(memory_space=pltpu.HBM)
    vmem = pl.BlockSpec(memory_space=pltpu.VMEM)
    wide = basis_table(512)
    rows = np.arange(512).reshape(16, BLOCKS, 8).transpose(1, 0, 2).reshape(-1)
    tables_x = np.stack(halves(wide[rows]))
    tables = np.stack(halves(basis_table(256)))
    rows = np.arange(256).reshape(8, 2, 16).transpose(1, 0, 2).reshape(-1)
    tables_z = tables[:, rows]
    flat = jnp.transpose(species, (0, 2, 3, 1)).reshape(F * 512, 512)
    arrays = (flat, tables_x, tables, tables_z, coupling, symbol_x, symbol_y, symbol_z.reshape(1, 256))
    results = pl.pallas_call(
        kernel,
        out_shape=(
            pltpu.VMEM((F, 8 * (BLOCKS - 1), 32, 256), jnp.float32),
            pltpu.VMEM((2, 256, 256), jnp.bfloat16),
            pltpu.VMEM((F, 8, 32, 256), jnp.float32),
            pltpu.VMEM((F, 8, 32, 256), jnp.float32),
            pltpu.VMEM((2, 8, 32, 128), jnp.float32),
        ),
        in_specs=[hbm] * 8,
        out_specs=[vmem] * 5,
        scratch_shapes=[
            pltpu.VMEM((F * 4 * 512 + 32, 128), jnp.float32),
            pltpu.VMEM((2, 512, 512), jnp.bfloat16),
            pltpu.VMEM((2, 256, 256), jnp.bfloat16),
            pltpu.VMEM((F, 512, 512), jnp.bfloat16),
            pltpu.VMEM((F, 512, 512), jnp.bfloat16),
            pltpu.VMEM((F, BLOCKS, 2, 16, 8, 256), jnp.float32),
            pltpu.VMEM((F, BLOCKS, 2, 16, 8, 256), jnp.float32),
            pltpu.VMEM((272, 128), jnp.float32),
            pltpu.VMEM((128, 256), jnp.bfloat16),
            pltpu.VMEM((128, 256), jnp.bfloat16),
            pltpu.VMEM((F, BLOCKS, 2, 8, 32, 128), jnp.float32),
            pltpu.VMEM((F, BLOCKS, 2, 8, 32, 128), jnp.float32),
            pltpu.VMEM((256, 256), jnp.bfloat16),
            pltpu.VMEM((256, 256), jnp.bfloat16),
            pltpu.VMEM((2, F, 8, 32, 256), jnp.float32),
            pltpu.VMEM((32, 256), jnp.float32),
            pltpu.SMEM((F, F), jnp.float32),
            pltpu.SMEM((512,), jnp.float32),
            pltpu.SMEM((256,), jnp.float32),
            pltpu.VMEM((1, 256), jnp.float32),
            pltpu.SemaphoreType.DMA((F,)),
            pltpu.SemaphoreType.DMA((7,)),
            pltpu.SemaphoreType.DMA((BLOCKS,)),
            pltpu.SemaphoreType.DMA((F, BLOCKS, 2)),
            pltpu.SemaphoreType.DMA((BLOCKS,)),
            pltpu.SemaphoreType.DMA((F, BLOCKS)),
        ],
        compiler_params=pltpu.CompilerParams(
            collective_id=0, has_side_effects=True, vmem_limit_bytes=40 * 2**20
        ),
        name="transform",
    )(*(pltpu.with_memory_space_constraint(a, pltpu.HBM) for a in arrays))
    return pl.pallas_call(
        write_kernel,
        out_shape=jax.ShapeDtypeStruct((F, 32, 32, 256), jnp.float32),
        in_specs=[vmem] * 5,
        out_specs=hbm,
        scratch_shapes=[
            pltpu.VMEM((F, 8, 32, 256), jnp.float32),
            pltpu.VMEM((256, 256), jnp.bfloat16),
            pltpu.VMEM((256, 256), jnp.bfloat16),
            pltpu.SemaphoreType.DMA((2, F)),
        ],
        compiler_params=pltpu.CompilerParams(vmem_limit_bytes=4 * 2**20),
        name="write",
    )(*results)


def solution(mesh):
    in_specs = (P(None, None, "left", "right"), P(), P(), P(), P())
    out_specs = P(None, "left", "right", None)
    return jax.shard_map(body, mesh=mesh, in_specs=in_specs, out_specs=out_specs, check_vma=False)
```

```python
import jax
import jax.numpy as jnp
import numpy as np
from jax import lax
from jax.experimental import pallas as pl
from jax.experimental.pallas import tpu as pltpu
from jax.sharding import PartitionSpec as P

MESH = pl.DeviceIdType.MESH
F = 4
BLOCKS = 4
LAG = 5
AHEAD = 8
CHUNKS = 2 * F * BLOCKS
LAST = F * BLOCKS - 1

LEFT_STEPS = [(dz, dx) for dx in (2, 1, 3, 0) for dz in (2, 1, 3, 0) if (dz, dx) != (0, 0)]
RIGHT_STEPS = [(dy, dc) for dc in (0, 1) for dy in (2, 1, 3, 0) if (dy, dc) != (0, 0)]


def basis_table(count):
    rank = np.arange(count)
    angle = 2.0 * np.pi / count * (rank[:, None] * rank[None, :] % count)
    return ((np.cos(angle) + np.sin(angle)) * count**-0.5).astype(np.float32)


def halves(table):
    high = table.astype(jnp.bfloat16)
    low = (table - high.astype(np.float32)).astype(jnp.bfloat16)
    return high, low


def split(values):
    high = values.astype(jnp.bfloat16)
    return high, (values - high.astype(jnp.float32)).astype(jnp.bfloat16)


def dot_nt(a, b):
    return lax.dot_general(a, b, (((1,), (1,)), ((), ())), preferred_element_type=jnp.float32)


def dot_nn(a, b):
    return lax.dot_general(a, b, (((1,), (0,)), ((), ())), preferred_element_type=jnp.float32)


def gather_blocks(arrays, width):
    count = len(arrays)
    position = lax.broadcasted_iota(jnp.int32, arrays[0].shape, 1) // width
    moved = [arrays[-w % count] for w in range(count)]
    bit = 1
    while bit < count:
        odd = position // bit % 2 == 1
        moved = [jnp.where(odd, moved[(w - bit) % count], moved[w]) for w in range(count)]
        bit *= 2
    return [moved[0]] + [pltpu.roll(moved[w], 128 - width * w, 1) for w in range(1, count)]


def z_transform(pieces, h, g_high, g_low):
    for half in range(2):
        arrays = [pieces[half, i] for i in range(8)]
        for i, array in enumerate(gather_blocks(arrays, 16)):
            high, low = split(array)
            g_high[pl.ds(32 * i, 32), pl.ds(128 * half, 128)] = high
            g_low[pl.ds(32 * i, 32), pl.ds(128 * half, 128)] = low
    part = dot_nn(g_high[...], h[0])
    part += dot_nn(g_low[...], h[0])
    part += dot_nn(g_high[...], h[1])
    return part.reshape(8, 32, 256)


def kernel(
    species, tables_x, tables, tables_z, coupling, symbol_x, symbol_y, symbol_z, out, hz, partial, slope, tail,
    grid, hx, h, d_high, d_low, s1, r1, d2, e_high, e_low, s2, r2, g_high, g_low, modes, base, mix, sx, sy, sz,
    in_sem, h_sem, send1, recv1, send2, recv2,
):
    left, right = lax.axis_index("left"), lax.axis_index("right")
    z, x = left // 4, left % 4
    y, core = right // 2, right % 2
    left_peers = [lax.rem(z + dz, 4) * 4 + lax.rem(x + dx, 4) for dz, dx in LEFT_STEPS]
    right_peers = [lax.rem(y + dy, 4) * 2 + lax.rem(core + dc, 2) for dy, dc in RIGHT_STEPS]

    barrier = pltpu.get_barrier_semaphore()
    for peer in left_peers:
        pl.semaphore_signal(barrier, inc=1, device_id=(peer, right), device_id_type=MESH)
    for peer in right_peers:
        pl.semaphore_signal(barrier, inc=1, device_id=(left, peer), device_id_type=MESH)

    def load(f, t):
        return pltpu.make_async_copy(
            species.at[pl.ds(512 * f, 512), pl.ds(128 * t, 128)],
            grid.at[pl.ds((4 * f + t) * 512, 512)],
            in_sem.at[f],
        )

    def loaded(f):
        rows = pl.ds(2048 * f, 2048)
        pltpu.make_async_copy(grid.at[rows], grid.at[rows], in_sem.at[f]).wait()

    small = [
        pltpu.make_async_copy(a, b, h_sem.at[i])
        for i, (a, b) in enumerate(
            [(tables_x, hx), (tables, h), (tables_z, hz), (coupling, mix), (symbol_x, sx), (symbol_y, sy), (symbol_z, sz)]
        )
    ]
    for t in range(4):
        load(0, t).start()
    small[0].start()
    for f in range(1, F):
        for t in range(4):
            load(f, t).start()
    for copy in small[1:]:
        copy.start()

    def first(f, b, half, k):
        return pltpu.make_async_remote_copy(
            src_ref=s1.at[f, b, half, left_peers[k]],
            dst_ref=r1.at[f, b, half, left],
            send_sem=send1.at[b],
            recv_sem=recv1.at[f, b % 2, half],
            device_id=(left_peers[k], right),
            device_id_type=MESH,
        )

    def second(f, b, half, k):
        return pltpu.make_async_remote_copy(
            src_ref=s2.at[f, b, half, right_peers[k]],
            dst_ref=r2.at[f, b, half, right],
            send_sem=send2.at[b],
            recv_sem=recv2.at[f, b % 2],
            device_id=(left, right_peers[k]),
            device_id_type=MESH,
        )

    def all_first(f, b, half):
        return pltpu.make_async_remote_copy(
            src_ref=s1.at[f, b, half, pl.ds(0, 15)],
            dst_ref=r1.at[f, b, half, pl.ds(0, 15)],
            send_sem=send1.at[b],
            recv_sem=recv1.at[f, b % 2, half],
            device_id=(left_peers[0], right),
            device_id_type=MESH,
        )

    def all_second(f, b):
        return pltpu.make_async_remote_copy(
            src_ref=s2.at[f, b, :, pl.ds(0, 7)],
            dst_ref=r2.at[f, b, :, pl.ds(0, 7)],
            send_sem=send2.at[b],
            recv_sem=recv2.at[f, b % 2],
            device_id=(left, right_peers[0]),
            device_id_type=MESH,
        )

    def send_first(c):
        for k in range(len(left_peers)):
            first(c // 2 % F, c // (2 * F), c % 2, k).start()

    def sent(b):
        pltpu.make_async_remote_copy(
            src_ref=s1.at[:, b, :, pl.ds(0, 15)],
            dst_ref=r1.at[:, b, :, pl.ds(0, 15)],
            send_sem=send1.at[b],
            recv_sem=recv1.at[0, b % 2, 0],
            device_id=(left_peers[0], right),
            device_id_type=MESH,
        ).wait_send()
        pltpu.make_async_remote_copy(
            src_ref=s2.at[:, b, :, pl.ds(0, 7)],
            dst_ref=r2.at[:, b, :, pl.ds(0, 7)],
            send_sem=send2.at[b],
            recv_sem=recv2.at[0, b % 2],
            device_id=(left, right_peers[0]),
            device_id_type=MESH,
        ).wait_send()

    def arrange(f):
        loaded(f)
        for t in range(4):
            for zi in range(32):
                rows = grid[pl.ds((4 * f + t) * 512 + zi, 16, stride=32), :]
                high, low = split(rows)
                place = pl.multiple_of(16 * (zi // 8 * 8 + lax.rem(zi % 8 + left, 8)), 16)
                d_high[f, pl.ds(place, 16), pl.ds(128 * t, 128)] = high
                d_low[f, pl.ds(place, 16), pl.ds(128 * t, 128)] = low

    def along_x(f, p):
        rows = pl.ds(pl.multiple_of(256 * p, 256), 256)
        part = dot_nt(hx[0, rows, :], d_high[f])
        part += dot_nt(hx[0, rows, :], d_low[f])
        part += dot_nt(hx[1, rows, :], d_high[f])
        for half in range(2):
            s1[f, pl.ds(2 * p, 2), half] = part[:, 256 * half : 256 * half + 256].reshape(2, 16, 8, 256)
            for i in range(2):
                r1[f, 2 * p + i, half, left] = s1[f, 2 * p + i, half, left]

    def opening(f, carry):
        arrange(f)

        @pl.when(f == 0)
        def _():
            small[0].wait()

        along_x(f, 0)

        @pl.when(f == 0)
        def _():
            pl.semaphore_wait(barrier, len(left_peers) + len(right_peers))

        send_first(2 * f)
        send_first(2 * f + 1)
        return carry

    def along_y(f, b, half):
        all_first(f, b, half).wait_recv()
        for t in range(2):
            for g in range(2):
                arrays = [r1[f, b, half, 8 * g + i, :, pl.ds(128 * t, 128)] for i in range(8)]
                for i, array in enumerate(gather_blocks(arrays, 16)):
                    d2[pl.ds(128 * g + 8 * (8 * t + i), 8), :] = array
        for g in range(2):
            for kx in range(8):
                high, low = split(d2[pl.ds(128 * g + kx, 16, stride=8), :])
                place = pl.multiple_of(16 * lax.rem(kx + right, 8), 16)
                e_high[pl.ds(place, 16), pl.ds(128 * g, 128)] = high
                e_low[pl.ds(place, 16), pl.ds(128 * g, 128)] = low
        both = dot_nt(h[...].reshape(512, 256), e_high[...])
        part = both[:256] + both[256:] + dot_nt(h[0], e_low[...])
        s2[f, b, half] = part.reshape(8, 32, 128)
        for k in range(len(right_peers)):
            second(f, b, half, k).start()
        r2[f, b, half, right] = s2[f, b, half, right]

    def along_z(f, b):
        all_second(f, b).wait_recv()
        modes[b % 2, f] = z_transform(r2.at[f, b], hz, g_high, g_low)

    def mixing(b, kx):
        weights = [[mix[a, c] for c in range(F)] for a in range(F)]
        shift = sx[32 * left + 8 * b + kx]
        for part in range(4):
            rows = pl.ds(8 * part, 8)
            weight = 1.0 / (base[rows, :] + shift)
            other = 1.0 - weight
            old = [modes[b % 2, a, kx, rows, :] for a in range(F)]
            for a in range(F):
                mixed = weights[a][0] * old[0]
                for c in range(1, F):
                    mixed += weights[a][c] * old[c]
                out[a, 8 * b + kx, rows, :] = weight * old[a] + other * mixed

    def prepare_last():
        weights = [[mix[a, c] for c in range(F)] for a in range(F)]

        def plane(kx, carry):
            shift = sx[32 * left + 8 * (BLOCKS - 1) + kx]
            for part in range(4):
                rows = pl.ds(8 * part, 8)
                weight = 1.0 / (base[rows, :] + shift)
                other = 1.0 - weight
                old = [modes[(BLOCKS - 1) % 2, a, kx, rows, :] for a in range(F - 1)]
                for a in range(F):
                    mixed = weights[a][0] * old[0]
                    for c in range(1, F - 1):
                        mixed += weights[a][c] * old[c]
                    first_terms = other * mixed
                    last_term = weights[a][F - 1] * other
                    if a < F - 1:
                        partial[a, kx, rows, :] = weight * old[a] + first_terms
                        slope[a, kx, rows, :] = last_term
                    else:
                        partial[a, kx, rows, :] = first_terms
                        slope[a, kx, rows, :] = last_term + weight
            return carry

        lax.fori_loop(0, 8, plane, 0)

    lax.fori_loop(0, F, opening, 0)

    def send_chunk(c, carry):
        send_first(c)
        return carry

    lax.fori_loop(2 * F, AHEAD, send_chunk, 0)
    small[1].wait()

    def step(i, carry):
        @pl.when(i < CHUNKS)
        def _():
            along_y(i // 2 % F, i // (2 * F), i % 2)

        @pl.when(i < F)
        def _():
            along_x(i, 1)

        @pl.when(i + AHEAD < CHUNKS)
        def _():
            send_first(i + AHEAD)

        @pl.when(i == F)
        def _():
            for copy in small[2:]:
                copy.wait()
            for ky in range(32):
                base[pl.ds(ky, 1), :] = 1.0 + (sz[...] + sy[32 * right + ky])

        @pl.when(((i + LAG) % 2 == 1) & (i > LAG) & (i < 2 * LAST + LAG))
        def _():
            j = (i - LAG - 1) // 2
            along_z(j % F, j // F)

        plane = i - 2 * F - LAG

        @pl.when(plane >= 0)
        def _():
            mixing(plane // 8, plane % 8)

        return carry

    lax.fori_loop(0, CHUNKS + LAG, step, 0)
    prepare_last()
    for b in range(BLOCKS):
        sent(b)
    all_second(F - 1, BLOCKS - 1).wait_recv()
    tail[...] = r2[F - 1, BLOCKS - 1]


def write_kernel(modes, h, partial, slope, tail, out, last, g_high, g_low, sems):
    done = 8 * (BLOCKS - 1)
    copies = [
        pltpu.make_async_copy(modes.at[f], out.at[f, pl.ds(0, done)], sems.at[0, f]) for f in range(F)
    ]
    for copy in copies:
        copy.start()
    last[F - 1] = z_transform(tail, h, g_high, g_low)
    for kx in range(8):
        for part in range(4):
            rows = pl.ds(8 * part, 8)
            old = last[F - 1, kx, rows, :]
            for a in range(F):
                last[a, kx, rows, :] = partial[a, kx, rows, :] + slope[a, kx, rows, :] * old
    for f in range(F):
        copies.append(pltpu.make_async_copy(last.at[f], out.at[f, pl.ds(done, 8)], sems.at[1, f]))
        copies[-1].start()
    for copy in copies:
        copy.wait()


def body(species, coupling, symbol_x, symbol_y, symbol_z):
    hbm = pl.BlockSpec(memory_space=pltpu.HBM)
    vmem = pl.BlockSpec(memory_space=pltpu.VMEM)
    wide = basis_table(512)
    rows = np.arange(512).reshape(16, BLOCKS, 8).transpose(1, 0, 2).reshape(-1)
    tables_x = np.stack(halves(wide[rows]))
    tables = np.stack(halves(basis_table(256)))
    rows = np.arange(256).reshape(8, 2, 16).transpose(1, 0, 2).reshape(-1)
    tables_z = tables[:, rows]
    flat = jnp.transpose(species, (0, 2, 3, 1)).reshape(F * 512, 512)
    arrays = (flat, tables_x, tables, tables_z, coupling, symbol_x, symbol_y, symbol_z.reshape(1, 256))
    results = pl.pallas_call(
        kernel,
        out_shape=(
            pltpu.VMEM((F, 8 * (BLOCKS - 1), 32, 256), jnp.float32),
            pltpu.VMEM((2, 256, 256), jnp.bfloat16),
            pltpu.VMEM((F, 8, 32, 256), jnp.float32),
            pltpu.VMEM((F, 8, 32, 256), jnp.float32),
            pltpu.VMEM((2, 8, 32, 128), jnp.float32),
        ),
        in_specs=[hbm] * 8,
        out_specs=[vmem] * 5,
        scratch_shapes=[
            pltpu.VMEM((F * 4 * 512 + 32, 128), jnp.float32),
            pltpu.VMEM((2, 512, 512), jnp.bfloat16),
            pltpu.VMEM((2, 256, 256), jnp.bfloat16),
            pltpu.VMEM((F, 512, 512), jnp.bfloat16),
            pltpu.VMEM((F, 512, 512), jnp.bfloat16),
            pltpu.VMEM((F, BLOCKS, 2, 16, 8, 256), jnp.float32),
            pltpu.VMEM((F, BLOCKS, 2, 16, 8, 256), jnp.float32),
            pltpu.VMEM((272, 128), jnp.float32),
            pltpu.VMEM((128, 256), jnp.bfloat16),
            pltpu.VMEM((128, 256), jnp.bfloat16),
            pltpu.VMEM((F, BLOCKS, 2, 8, 32, 128), jnp.float32),
            pltpu.VMEM((F, BLOCKS, 2, 8, 32, 128), jnp.float32),
            pltpu.VMEM((256, 256), jnp.bfloat16),
            pltpu.VMEM((256, 256), jnp.bfloat16),
            pltpu.VMEM((2, F, 8, 32, 256), jnp.float32),
            pltpu.VMEM((32, 256), jnp.float32),
            pltpu.SMEM((F, F), jnp.float32),
            pltpu.SMEM((512,), jnp.float32),
            pltpu.SMEM((256,), jnp.float32),
            pltpu.VMEM((1, 256), jnp.float32),
            pltpu.SemaphoreType.DMA((F,)),
            pltpu.SemaphoreType.DMA((7,)),
            pltpu.SemaphoreType.DMA((BLOCKS,)),
            pltpu.SemaphoreType.DMA((F, 2, 2)),
            pltpu.SemaphoreType.DMA((BLOCKS,)),
            pltpu.SemaphoreType.DMA((F, 2)),
        ],
        compiler_params=pltpu.CompilerParams(
            collective_id=0, has_side_effects=True, vmem_limit_bytes=40 * 2**20
        ),
        name="transform",
    )(*(pltpu.with_memory_space_constraint(a, pltpu.HBM) for a in arrays))
    return pl.pallas_call(
        write_kernel,
        out_shape=jax.ShapeDtypeStruct((F, 32, 32, 256), jnp.float32),
        in_specs=[vmem] * 5,
        out_specs=hbm,
        scratch_shapes=[
            pltpu.VMEM((F, 8, 32, 256), jnp.float32),
            pltpu.VMEM((256, 256), jnp.bfloat16),
            pltpu.VMEM((256, 256), jnp.bfloat16),
            pltpu.SemaphoreType.DMA((2, F)),
        ],
        compiler_params=pltpu.CompilerParams(vmem_limit_bytes=4 * 2**20),
        name="write",
    )(*results)


def solution(mesh):
    in_specs = (P(None, None, "left", "right"), P(), P(), P(), P())
    out_specs = P(None, "left", "right", None)
    return jax.shard_map(body, mesh=mesh, in_specs=in_specs, out_specs=out_specs, check_vma=False)
```

```python
import jax
import jax.numpy as jnp
import numpy as np
from jax import lax
from jax.experimental import pallas as pl
from jax.experimental.pallas import tpu as pltpu
from jax.sharding import PartitionSpec as P

MESH = pl.DeviceIdType.MESH
F = 4
BLOCKS = 4
LAG = 5
AHEAD = 8
CHUNKS = 2 * F * BLOCKS
LAST = F * BLOCKS - 1

LEFT_STEPS = [(dz, dx) for dx in (2, 1, 3, 0) for dz in (2, 1, 3, 0) if (dz, dx) != (0, 0)]
RIGHT_STEPS = [(dy, dc) for dc in (0, 1) for dy in (2, 1, 3, 0) if (dy, dc) != (0, 0)]


def basis_table(count):
    rank = np.arange(count)
    angle = 2.0 * np.pi / count * (rank[:, None] * rank[None, :] % count)
    return ((np.cos(angle) + np.sin(angle)) * count**-0.5).astype(np.float32)


def halves(table):
    high = table.astype(jnp.bfloat16)
    low = (table - high.astype(np.float32)).astype(jnp.bfloat16)
    return high, low


def split(values):
    high = values.astype(jnp.bfloat16)
    return high, (values - high.astype(jnp.float32)).astype(jnp.bfloat16)


def dot_nt(a, b):
    return lax.dot_general(a, b, (((1,), (1,)), ((), ())), preferred_element_type=jnp.float32)


def dot_nn(a, b):
    return lax.dot_general(a, b, (((1,), (0,)), ((), ())), preferred_element_type=jnp.float32)


def gather_blocks(arrays, width):
    count = len(arrays)
    position = lax.broadcasted_iota(jnp.int32, arrays[0].shape, 1) // width
    moved = [arrays[-w % count] for w in range(count)]
    bit = 1
    while bit < count:
        odd = position // bit % 2 == 1
        moved = [jnp.where(odd, moved[(w - bit) % count], moved[w]) for w in range(count)]
        bit *= 2
    return [moved[0]] + [pltpu.roll(moved[w], 128 - width * w, 1) for w in range(1, count)]


def z_transform(pieces, h, g_high, g_low):
    for half in range(2):
        arrays = [pieces[half, i] for i in range(8)]
        for i, array in enumerate(gather_blocks(arrays, 16)):
            high, low = split(array)
            g_high[pl.ds(32 * i, 32), pl.ds(128 * half, 128)] = high
            g_low[pl.ds(32 * i, 32), pl.ds(128 * half, 128)] = low
    part = dot_nn(g_high[...], h[0])
    part += dot_nn(g_low[...], h[0])
    part += dot_nn(g_high[...], h[1])
    return part.reshape(8, 32, 256)


def kernel(
    species, tables_x, tables, tables_z, coupling, symbol_x, symbol_y, symbol_z, out, hz, partial, slope, tail,
    grid, hx, h, d_high, d_low, s1, r1, d2, e_high, e_low, s2, r2, g_high, g_low, modes, base, mix, sx, sy, sz,
    in_sem, h_sem, send1, recv1, send2, recv2,
):
    left, right = lax.axis_index("left"), lax.axis_index("right")
    z, x = left // 4, left % 4
    y, core = right // 2, right % 2
    left_peers = [lax.rem(z + dz, 4) * 4 + lax.rem(x + dx, 4) for dz, dx in LEFT_STEPS]
    right_peers = [lax.rem(y + dy, 4) * 2 + lax.rem(core + dc, 2) for dy, dc in RIGHT_STEPS]

    barrier = pltpu.get_barrier_semaphore()
    for peer in left_peers:
        pl.semaphore_signal(barrier, inc=1, device_id=(peer, right), device_id_type=MESH)
    for peer in right_peers:
        pl.semaphore_signal(barrier, inc=1, device_id=(left, peer), device_id_type=MESH)

    def load(f, t):
        return pltpu.make_async_copy(
            species.at[pl.ds(512 * f, 512), pl.ds(128 * t, 128)],
            grid.at[pl.ds((4 * f + t) * 512, 512)],
            in_sem.at[f],
        )

    def loaded(f):
        rows = pl.ds(2048 * f, 2048)
        pltpu.make_async_copy(grid.at[rows], grid.at[rows], in_sem.at[f]).wait()

    small = [
        pltpu.make_async_copy(a, b, h_sem.at[i])
        for i, (a, b) in enumerate(
            [(tables_x, hx), (tables, h), (tables_z, hz), (coupling, mix), (symbol_x, sx), (symbol_y, sy), (symbol_z, sz)]
        )
    ]
    for t in range(4):
        load(0, t).start()
    small[0].start()
    for f in range(1, F):
        for t in range(4):
            load(f, t).start()
    for copy in small[1:]:
        copy.start()

    def first(f, b, half, k):
        return pltpu.make_async_remote_copy(
            src_ref=s1.at[f, b, half, left_peers[k]],
            dst_ref=r1.at[f, b, half, left],
            send_sem=send1.at[b],
            recv_sem=recv1.at[f, b, half],
            device_id=(left_peers[k], right),
            device_id_type=MESH,
        )

    def second(f, b, half, k):
        return pltpu.make_async_remote_copy(
            src_ref=s2.at[f, b, half, right_peers[k]],
            dst_ref=r2.at[f, b, half, right],
            send_sem=send2.at[b],
            recv_sem=recv2.at[f, b],
            device_id=(left, right_peers[k]),
            device_id_type=MESH,
        )

    def all_first(f, b, half):
        return pltpu.make_async_remote_copy(
            src_ref=s1.at[f, b, half, pl.ds(0, 15)],
            dst_ref=r1.at[f, b, half, pl.ds(0, 15)],
            send_sem=send1.at[b],
            recv_sem=recv1.at[f, b, half],
            device_id=(left_peers[0], right),
            device_id_type=MESH,
        )

    def all_second(f, b):
        return pltpu.make_async_remote_copy(
            src_ref=s2.at[f, b, :, pl.ds(0, 7)],
            dst_ref=r2.at[f, b, :, pl.ds(0, 7)],
            send_sem=send2.at[b],
            recv_sem=recv2.at[f, b],
            device_id=(left, right_peers[0]),
            device_id_type=MESH,
        )

    def send_first(c):
        for k in range(len(left_peers)):
            first(c // 2 % F, c // (2 * F), c % 2, k).start()

    def sent(b):
        pltpu.make_async_remote_copy(
            src_ref=s1.at[:, b, :, pl.ds(0, 15)],
            dst_ref=r1.at[:, b, :, pl.ds(0, 15)],
            send_sem=send1.at[b],
            recv_sem=recv1.at[0, b, 0],
            device_id=(left_peers[0], right),
            device_id_type=MESH,
        ).wait_send()
        pltpu.make_async_remote_copy(
            src_ref=s2.at[:, b, :, pl.ds(0, 7)],
            dst_ref=r2.at[:, b, :, pl.ds(0, 7)],
            send_sem=send2.at[b],
            recv_sem=recv2.at[0, b],
            device_id=(left, right_peers[0]),
            device_id_type=MESH,
        ).wait_send()

    def arrange(f):
        loaded(f)
        for t in range(4):
            for zi in range(32):
                rows = grid[pl.ds((4 * f + t) * 512 + zi, 16, stride=32), :]
                high, low = split(rows)
                place = pl.multiple_of(16 * (zi // 8 * 8 + lax.rem(zi % 8 + left, 8)), 16)
                d_high[f, pl.ds(place, 16), pl.ds(128 * t, 128)] = high
                d_low[f, pl.ds(place, 16), pl.ds(128 * t, 128)] = low

    def along_x(f, p):
        rows = pl.ds(pl.multiple_of(256 * p, 256), 256)
        part = dot_nt(hx[0, rows, :], d_high[f])
        part += dot_nt(hx[0, rows, :], d_low[f])
        part += dot_nt(hx[1, rows, :], d_high[f])
        for half in range(2):
            s1[f, pl.ds(2 * p, 2), half] = part[:, 256 * half : 256 * half + 256].reshape(2, 16, 8, 256)
            for i in range(2):
                r1[f, 2 * p + i, half, left] = s1[f, 2 * p + i, half, left]

    def opening(f, carry):
        arrange(f)

        @pl.when(f == 0)
        def _():
            small[0].wait()

        along_x(f, 0)

        @pl.when(f == 0)
        def _():
            pl.semaphore_wait(barrier, len(left_peers) + len(right_peers))

        send_first(2 * f)
        send_first(2 * f + 1)
        return carry

    def along_y(f, b, half):
        all_first(f, b, half).wait_recv()
        for t in range(2):
            for g in range(2):
                arrays = [r1[f, b, half, 8 * g + i, :, pl.ds(128 * t, 128)] for i in range(8)]
                for i, array in enumerate(gather_blocks(arrays, 16)):
                    d2[pl.ds(128 * g + 8 * (8 * t + i), 8), :] = array
        for g in range(2):
            for kx in range(8):
                high, low = split(d2[pl.ds(128 * g + kx, 16, stride=8), :])
                place = pl.multiple_of(16 * lax.rem(kx + right, 8), 16)
                e_high[pl.ds(place, 16), pl.ds(128 * g, 128)] = high
                e_low[pl.ds(place, 16), pl.ds(128 * g, 128)] = low
        for dy in (2, 1, 3, 0):
            chip = lax.rem(y + dy, 4)
            rows = pl.ds(pl.multiple_of(64 * chip, 64), 64)
            part = dot_nt(h[0, rows, :], e_high[...])
            part += dot_nt(h[0, rows, :], e_low[...])
            part += dot_nt(h[1, rows, :], e_high[...])
            s2[f, b, half, pl.ds(2 * chip, 2)] = part.reshape(2, 32, 128)
            for k, (step_y, _) in enumerate(RIGHT_STEPS):
                if step_y == dy:
                    second(f, b, half, k).start()
        r2[f, b, half, right] = s2[f, b, half, right]

    def along_z(f, b):
        all_second(f, b).wait_recv()
        modes[b % 2, f] = z_transform(r2.at[f, b], hz, g_high, g_low)

    def mixing(b, kx):
        weights = [[mix[a, c] for c in range(F)] for a in range(F)]
        shift = sx[32 * left + 8 * b + kx]
        for part in range(4):
            rows = pl.ds(8 * part, 8)
            weight = 1.0 / (base[rows, :] + shift)
            other = 1.0 - weight
            old = [modes[b % 2, a, kx, rows, :] for a in range(F)]
            for a in range(F):
                mixed = weights[a][0] * old[0]
                for c in range(1, F):
                    mixed += weights[a][c] * old[c]
                out[a, 8 * b + kx, rows, :] = weight * old[a] + other * mixed

    def prepare_last():
        weights = [[mix[a, c] for c in range(F)] for a in range(F)]

        def plane(kx, carry):
            shift = sx[32 * left + 8 * (BLOCKS - 1) + kx]
            for part in range(4):
                rows = pl.ds(8 * part, 8)
                weight = 1.0 / (base[rows, :] + shift)
                other = 1.0 - weight
                old = [modes[(BLOCKS - 1) % 2, a, kx, rows, :] for a in range(F - 1)]
                for a in range(F):
                    mixed = weights[a][0] * old[0]
                    for c in range(1, F - 1):
                        mixed += weights[a][c] * old[c]
                    first_terms = other * mixed
                    last_term = weights[a][F - 1] * other
                    if a < F - 1:
                        partial[a, kx, rows, :] = weight * old[a] + first_terms
                        slope[a, kx, rows, :] = last_term
                    else:
                        partial[a, kx, rows, :] = first_terms
                        slope[a, kx, rows, :] = last_term + weight
            return carry

        lax.fori_loop(0, 8, plane, 0)

    lax.fori_loop(0, F, opening, 0)

    def send_chunk(c, carry):
        send_first(c)
        return carry

    lax.fori_loop(2 * F, AHEAD, send_chunk, 0)
    small[1].wait()

    def step(i, carry):
        @pl.when(i < CHUNKS)
        def _():
            along_y(i // 2 % F, i // (2 * F), i % 2)

        @pl.when(i < F)
        def _():
            along_x(i, 1)

        @pl.when(i + AHEAD < CHUNKS)
        def _():
            send_first(i + AHEAD)

        @pl.when(i == F)
        def _():
            for copy in small[2:]:
                copy.wait()
            for ky in range(32):
                base[pl.ds(ky, 1), :] = 1.0 + (sz[...] + sy[32 * right + ky])

        @pl.when(((i + LAG) % 2 == 1) & (i > LAG) & (i < 2 * LAST + LAG))
        def _():
            j = (i - LAG - 1) // 2
            along_z(j % F, j // F)

        plane = i - 2 * F - LAG

        @pl.when(plane >= 0)
        def _():
            mixing(plane // 8, plane % 8)

        return carry

    lax.fori_loop(0, CHUNKS + LAG, step, 0)
    prepare_last()
    for b in range(BLOCKS):
        sent(b)
    all_second(F - 1, BLOCKS - 1).wait_recv()
    tail[...] = r2[F - 1, BLOCKS - 1]


def write_kernel(modes, h, partial, slope, tail, out, last, g_high, g_low, sems):
    done = 8 * (BLOCKS - 1)
    copies = [
        pltpu.make_async_copy(modes.at[f], out.at[f, pl.ds(0, done)], sems.at[0, f]) for f in range(F)
    ]
    for copy in copies:
        copy.start()
    last[F - 1] = z_transform(tail, h, g_high, g_low)
    for kx in range(8):
        for part in range(4):
            rows = pl.ds(8 * part, 8)
            old = last[F - 1, kx, rows, :]
            for a in range(F):
                last[a, kx, rows, :] = partial[a, kx, rows, :] + slope[a, kx, rows, :] * old
    for f in range(F):
        copies.append(pltpu.make_async_copy(last.at[f], out.at[f, pl.ds(done, 8)], sems.at[1, f]))
        copies[-1].start()
    for copy in copies:
        copy.wait()


def body(species, coupling, symbol_x, symbol_y, symbol_z):
    hbm = pl.BlockSpec(memory_space=pltpu.HBM)
    vmem = pl.BlockSpec(memory_space=pltpu.VMEM)
    wide = basis_table(512)
    rows = np.arange(512).reshape(16, BLOCKS, 8).transpose(1, 0, 2).reshape(-1)
    tables_x = np.stack(halves(wide[rows]))
    tables = np.stack(halves(basis_table(256)))
    rows = np.arange(256).reshape(8, 2, 16).transpose(1, 0, 2).reshape(-1)
    tables_z = tables[:, rows]
    flat = jnp.transpose(species, (0, 2, 3, 1)).reshape(F * 512, 512)
    arrays = (flat, tables_x, tables, tables_z, coupling, symbol_x, symbol_y, symbol_z.reshape(1, 256))
    results = pl.pallas_call(
        kernel,
        out_shape=(
            pltpu.VMEM((F, 8 * (BLOCKS - 1), 32, 256), jnp.float32),
            pltpu.VMEM((2, 256, 256), jnp.bfloat16),
            pltpu.VMEM((F, 8, 32, 256), jnp.float32),
            pltpu.VMEM((F, 8, 32, 256), jnp.float32),
            pltpu.VMEM((2, 8, 32, 128), jnp.float32),
        ),
        in_specs=[hbm] * 8,
        out_specs=[vmem] * 5,
        scratch_shapes=[
            pltpu.VMEM((F * 4 * 512 + 32, 128), jnp.float32),
            pltpu.VMEM((2, 512, 512), jnp.bfloat16),
            pltpu.VMEM((2, 256, 256), jnp.bfloat16),
            pltpu.VMEM((F, 512, 512), jnp.bfloat16),
            pltpu.VMEM((F, 512, 512), jnp.bfloat16),
            pltpu.VMEM((F, BLOCKS, 2, 16, 8, 256), jnp.float32),
            pltpu.VMEM((F, BLOCKS, 2, 16, 8, 256), jnp.float32),
            pltpu.VMEM((272, 128), jnp.float32),
            pltpu.VMEM((128, 256), jnp.bfloat16),
            pltpu.VMEM((128, 256), jnp.bfloat16),
            pltpu.VMEM((F, BLOCKS, 2, 8, 32, 128), jnp.float32),
            pltpu.VMEM((F, BLOCKS, 2, 8, 32, 128), jnp.float32),
            pltpu.VMEM((256, 256), jnp.bfloat16),
            pltpu.VMEM((256, 256), jnp.bfloat16),
            pltpu.VMEM((2, F, 8, 32, 256), jnp.float32),
            pltpu.VMEM((32, 256), jnp.float32),
            pltpu.SMEM((F, F), jnp.float32),
            pltpu.SMEM((512,), jnp.float32),
            pltpu.SMEM((256,), jnp.float32),
            pltpu.VMEM((1, 256), jnp.float32),
            pltpu.SemaphoreType.DMA((F,)),
            pltpu.SemaphoreType.DMA((7,)),
            pltpu.SemaphoreType.DMA((BLOCKS,)),
            pltpu.SemaphoreType.DMA((F, BLOCKS, 2)),
            pltpu.SemaphoreType.DMA((BLOCKS,)),
            pltpu.SemaphoreType.DMA((F, BLOCKS)),
        ],
        compiler_params=pltpu.CompilerParams(
            collective_id=0, has_side_effects=True, vmem_limit_bytes=40 * 2**20
        ),
        name="transform",
    )(*(pltpu.with_memory_space_constraint(a, pltpu.HBM) for a in arrays))
    return pl.pallas_call(
        write_kernel,
        out_shape=jax.ShapeDtypeStruct((F, 32, 32, 256), jnp.float32),
        in_specs=[vmem] * 5,
        out_specs=hbm,
        scratch_shapes=[
            pltpu.VMEM((F, 8, 32, 256), jnp.float32),
            pltpu.VMEM((256, 256), jnp.bfloat16),
            pltpu.VMEM((256, 256), jnp.bfloat16),
            pltpu.SemaphoreType.DMA((2, F)),
        ],
        compiler_params=pltpu.CompilerParams(vmem_limit_bytes=4 * 2**20),
        name="write",
    )(*results)


def solution(mesh):
    in_specs = (P(None, None, "left", "right"), P(), P(), P(), P())
    out_specs = P(None, "left", "right", None)
    return jax.shard_map(body, mesh=mesh, in_specs=in_specs, out_specs=out_specs, check_vma=False)
```
